1024 devices in a mesh: row: 64 (over x, z), col: 16 (over y, core).
Axes of the slice: x: 8, y: 8, z: 8, core: 2. Of those that a mesh axis runs over, the one named last changes fastest.
Arguments:
- rhs: bfloat16 [2, 32768, 8192], P(None, 'row', 'col'), may hold values from -6 to 6
- panel: bfloat16 [2, 32768, 1024], P(None, 'row', 'col'), may hold values from -0.25 to 0.25
- pivots: float32 [1024], P('col'), may hold values from 2 to 4
Outputs:
- updated: float32 [2, 32768, 8192], P(None, 'row', 'col')
The draws below stay inside these ranges and needn't reach their ends.
All inputs are finite; a program needn't handle non-finite values.
Results may differ from the reference program's by a relative error of at most 0.0045.
Values may be sent and summed in bfloat16 or wider, within the bound.
A program may use at most 32 MiB of HBM per device.

```python
import math
import jax
import jax.numpy as jnp
from jax import lax

BLK = 512
T_DEV = 2
COLS_DEV = 512
ROWS = 32768
COLS = 8192


def steps_of(stream_key, dims, cuts, least, largest):
    loudness = 1.0
    for axis_at, blocks in cuts:
        draws = jax.random.uniform(jax.random.fold_in(jax.random.fold_in(stream_key, 6), axis_at), (blocks,), jnp.float32, least / len(cuts), largest / len(cuts))
        loudness = loudness * jnp.repeat(jnp.exp(draws), dims[axis_at] // blocks).reshape((-1,) + (1,) * (len(dims) - 1 - axis_at))
    return loudness


def scatter_about(key, shape, scale, limit, cuts=(), held_as=jnp.bfloat16):
    entries = scale * jax.random.normal(key, shape, jnp.float32)
    if cuts:
        entries = entries * steps_of(key, shape, cuts, -0.22, 0.18)
    return jnp.clip(entries, -limit, limit).astype(held_as)


def setup_inputs(seed: int = 0) -> dict:
    seeds = jax.random.split(jax.random.key(seed), 4)
    rhs = scatter_about(seeds[0], (T_DEV, ROWS, COLS), 1.0, 6.0, ((1, 64), (2, 16)))
    panel = scatter_about(seeds[1], (T_DEV, ROWS, 2 * BLK), BLK ** -0.5, 0.25, ((1, 64), (2, 16)))
    pivots = jnp.clip(jnp.exp(math.log(4.0) - 0.6931472 * jax.random.uniform(seeds[2], (2 * BLK,), jnp.float32) ** steps_of(seeds[2], (2 * BLK,), ((0, 16),), -0.2, 0.2)), 2.0, 4.0)
    return dict(rhs=rhs, panel=panel, pivots=pivots)


def lower_solve(matrix, values):
    return lax.linalg.triangular_solve(matrix, values, left_side=True, lower=True)

def reference(rhs, panel, pivots):
    layers = rhs.shape[0]
    rows = rhs.shape[1]
    cols = rhs.shape[2]
    left = panel.reshape(layers * rows, 2 * BLK)
    lower_zero = jnp.tril(panel[0, 0:BLK, 0:BLK].astype(jnp.float32), -1) + jnp.diag(pivots[0:BLK])
    lower_one = jnp.tril(panel[0, BLK:2 * BLK, BLK:2 * BLK].astype(jnp.float32), -1) + jnp.diag(pivots[BLK:2 * BLK])
    width = COLS_DEV
    blocks = cols // width
    stacked = rhs.reshape(layers * rows, blocks, width).transpose(1, 0, 2)

    def solve_block(block):
        values = block.astype(jnp.float32)
        first = lower_solve(lower_zero, values[0:BLK])
        first_low = first.astype(jnp.bfloat16)
        values = values - jnp.dot(left[:, 0:BLK].astype(jnp.float32), first_low.astype(jnp.float32), preferred_element_type=jnp.float32)
        second = lower_solve(lower_one, values[BLK:2 * BLK])
        second_low = second.astype(jnp.bfloat16)
        values = values - jnp.dot(left[:, BLK:2 * BLK].astype(jnp.float32), second_low.astype(jnp.float32), preferred_element_type=jnp.float32)
        values = values.at[0:BLK].set(first)
        values = values.at[BLK:2 * BLK].set(second)
        return values
    solved = lax.map(solve_block, stacked)
    return solved.transpose(1, 0, 2).reshape(layers, rows, cols)
```

```python
import functools

import jax
import jax.numpy as jnp
from jax import lax
from jax.experimental import pallas as pl
from jax.experimental.pallas import tpu as pltpu
from jax.sharding import Mesh
from jax.sharding import PartitionSpec as P

MESH = pl.DeviceIdType.MESH
F32 = jnp.float32
BF16 = jnp.bfloat16
X, Z, Y, CORE = "row_0", "row_1", "col_0", "col_1"
RING = 8
PLANE, RIDGE = 1, 0
ROUNDS = 8
DEEP = 256 // ROUNDS
LAG = 3


def dot(a, b):
    return jnp.dot(a, b, preferred_element_type=F32)


def split(v):
    high = v.astype(BF16)
    return high, (v - high.astype(F32)).astype(BF16)


def dot_exact_left(a, b):
    high, low = split(b)
    return dot(a, high) + dot(a, low)


def dot_exact_right(a, b):
    high, low = split(a)
    return dot(high, b) + dot(low, b)


def dot_both(a, b):
    ah, al = split(a)
    bh, bl = split(b)
    return dot(ah, bh) + (dot(ah, bl) + dot(al, bh))


def iota(shape, dim):
    return lax.broadcasted_iota(jnp.int32, shape, dim)


def invert_diagonal(block, pivots):
    n, base = 128, 32
    rows, cols = iota((n, n), 0), iota((n, n), 1)
    raw = jnp.where(rows > cols, block.astype(F32), 0.0)
    inverse_row = 1.0 / pivots
    inverse_col = jnp.sum(jnp.where(rows == cols, inverse_row, 0.0), axis=1, keepdims=True)
    scaled = raw * inverse_col
    parts = []
    for at in range(0, n, base):
        lower = scaled[at : at + base, :]
        part = (iota((base, n), 0) + at == iota((base, n), 1)).astype(F32)
        for j in range(base - 1):
            part = part - lower[:, at + j : at + j + 1] * part[j : j + 1, :]
        parts.append(part)
    result = jnp.concatenate(parts, axis=0)
    inside = rows // base == cols // base
    result = jnp.where(inside, result, 0.0) * inverse_row
    size = base
    while size < n:
        below = (rows // size) % 2 == 1
        mask = below & (cols // size == rows // size - 1)
        link = jnp.where(mask, raw, 0.0).astype(BF16)
        result = result - dot_both(result, dot_exact_left(link, result))
        size *= 2
    return result


def kernel(
    rhs_hbm, panel_hbm, pivots_hbm, out_hbm,
    own, sibling_own, piv, sibling_piv, rhs, panel, sides, slabs, inverses, low, full, out,
    local_sem, pair_send, pair_recv,
    plane_send, plane_recv, hand_send, hand_recv,
    p_send, p_recv, p_hand_send, p_hand_recv,
    s_send, s_recv, s_hand_send, s_hand_recv,
):
    x, z, y, core = (lax.axis_index(name) for name in (X, Z, Y, CORE))
    row = x * RING + z
    is_plane = core == PLANE
    is_ridge = core == RIDGE

    def around(value, by):
        return lax.rem(value + by + RING, RING)

    def remote(src, dst, send, recv, where):
        return pltpu.make_async_remote_copy(
            src_ref=src, dst_ref=dst, send_sem=send, recv_sem=recv, device_id=where, device_id_type=MESH
        )

    mate = {CORE: 1 - core}

    take_panel = pltpu.make_async_copy(panel_hbm, own, local_sem.at[0])
    take_piv = pltpu.make_async_copy(pivots_hbm, piv, local_sem.at[1])
    take_rhs = pltpu.make_async_copy(rhs_hbm, rhs, local_sem.at[2])
    take_panel.start()
    take_piv.start()
    take_rhs.start()
    barrier = pltpu.get_barrier_semaphore()
    pl.semaphore_signal(barrier, inc=1, device_id=mate, device_id_type=MESH)

    @pl.when(is_plane)
    def _():
        for by in (1, -1):
            pl.semaphore_signal(barrier, inc=1, device_id={X: around(x, by)}, device_id_type=MESH)
            pl.semaphore_signal(barrier, inc=1, device_id={Z: around(z, by)}, device_id_type=MESH)
        pl.semaphore_wait(barrier, 5)

    @pl.when(is_ridge)
    def _():
        for by in (1, -1):
            pl.semaphore_signal(barrier, inc=1, device_id={Y: around(y, by)}, device_id_type=MESH)
        pl.semaphore_wait(barrier, 3)

    take_panel.wait()
    pair_panel = remote(own, sibling_own, pair_send.at[0], pair_recv.at[0], mate)
    pair_panel.start()
    take_piv.wait()
    pair_piv = remote(piv, sibling_piv, pair_send.at[1], pair_recv.at[1], mate)
    pair_piv.start()
    take_rhs.wait()
    pair_side = remote(rhs.at[0], sides.at[RIDGE, row], pair_send.at[2], pair_recv.at[2], mate)

    @pl.when((row < 2) & is_ridge)
    def _():
        pair_side.start()

    pair_panel.wait_recv()
    lane, place = iota((64, 128), 1), iota((64, 128), 0)
    mine = (lane == place + core * 64).astype(BF16)
    theirs = (lane == place + (1 - core) * 64).astype(BF16)
    for layer in range(2):
        chip = (dot(own[layer], mine) + dot(sibling_own[layer], theirs)).astype(BF16)
        panel[y, layer * 512 : (layer + 1) * 512, :] = chip

    def needed(kind, tile, tree, at):
        if kind == "R":
            return at >= 0
        if kind == "D":
            return at // 4 == tile
        if tile == 0:
            return (at == 0) if tree == 0 else (at < 3)
        return (at <= 4) if tree == 0 else (at < 7)

    def piece(kind, tile, tree, index, of=None):
        if kind == "R":
            rows = pl.ds(tree * 256 + index * DEEP, DEEP)
            return sides.at[:, tile, rows, :] if of is None else sides.at[of, tile, rows, :]
        if kind == "D":
            return inverses.at[y, tree * 64 : (tree + 1) * 64, :]
        if tile == 0:
            return slabs.at[0, y, 128:256, :] if tree == 0 else slabs.at[0, y, 256:512, :]
        return slabs.at[1, y, 0:256, :] if tree == 0 else slabs.at[1, y, 256:512, :]

    def slot_of(kind, index):
        return {"L": 0, "D": 1, "R": 2}[kind] + index

    first_of = (Z, X)
    second_of = (X, Z)

    def place_in(tile, tree):
        to_z = lax.rem(z - tile + RING, RING)
        return (to_z, x) if tree == 0 else (x, to_z)

    def roles(tile, tree):
        f, g = place_in(tile, tree)
        root = (f == 0) & (g == 0)
        late = (f == 0) & (g != 0)
        up_first = (g == 0) & (f <= 3)
        down_first = ((g == 0) & ((f == 0) | (f >= 6))) | ((f == 1) & (g != 0))
        up_second = (f != 0) & (g <= 3)
        down_second = (f != 0) & ((g == 0) | (g >= 6))
        return root, late, (up_first, down_first, up_second, down_second)

    def targets(tree):
        at = {X: x, Z: z}
        a, b = first_of[tree], second_of[tree]
        return [{a: around(at[a], 1)}, {a: around(at[a], -1)}, {b: around(at[b], 1)}, {b: around(at[b], -1)}]

    def plane_copy(kind, tile, tree, index, direction):
        ref = piece(kind, tile, tree, index)
        slot = slot_of(kind, index)
        return remote(
            ref, ref, plane_send.at[tile, tree, direction, slot], plane_recv.at[tile, tree, slot],
            targets(tree)[direction],
        )

    def hand_copy(kind, tile, tree, index):
        ref = piece(kind, tile, tree, index, of=RIDGE)
        slot = slot_of(kind, index)
        return remote(ref, ref, hand_send.at[tile, tree, slot], hand_recv.at[tile, tree, slot], mate)

    def hands(kind, root):
        return jnp.logical_not(root) if kind == "R" else (row >= 0)

    def relay(kind, index, late_turn):
        for tile in range(2):
            for tree in range(2):
                root, late, sends = roles(tile, tree)
                want = needed(kind, tile, tree, y)
                turn = late if late_turn else jnp.logical_not(late)

                @pl.when(want & turn)
                def _(tile=tile, tree=tree, root=root, sends=sends):
                    @pl.when(jnp.logical_not(root))
                    def _():
                        plane_copy(kind, tile, tree, index, 0).wait_recv()

                    if not late_turn:
                        for direction in range(4):

                            @pl.when(sends[direction])
                            def _(direction=direction):
                                plane_copy(kind, tile, tree, index, direction).start()

                    @pl.when(hands(kind, root))
                    def _():
                        hand_copy(kind, tile, tree, index).start()

    def drain(kind, index):
        for tile in range(2):
            for tree in range(2):
                root, late, sends = roles(tile, tree)
                want = needed(kind, tile, tree, y)
                for direction in range(4):

                    @pl.when(want & sends[direction])
                    def _(tile=tile, tree=tree, direction=direction):
                        plane_copy(kind, tile, tree, index, direction).wait_send()

                @pl.when(want & hands(kind, root))
                def _(tile=tile, tree=tree):
                    hand_copy(kind, tile, tree, index).wait_send()

    def p_ref(source, layer):
        return panel.at[source, layer * 512 : (layer + 1) * 512, :]

    def s_ref(unit, source):
        if unit == 0:
            return slabs.at[1, source, 0:256, :]
        if unit == 1:
            return slabs.at[1, source, 256:512, :]
        if unit == 2:
            return slabs.at[0, source, 256:512, :]
        if unit == 3:
            return slabs.at[0, source, 128:256, :]
        return inverses.at[source]

    UNIT = {0: ("L", 1, 0), 1: ("L", 1, 1), 2: ("L", 0, 1), 3: ("L", 0, 0)}

    def s_needed(unit, source):
        return needed(*UNIT[unit], source) if unit < 4 else (source >= 0)

    class Ring:
        def __init__(self, ref, wanted, send, recv, hand_s, hand_r):
            self.ref, self.wanted = ref, wanted
            self.send, self.recv, self.hand_s, self.hand_r = send, recv, hand_s, hand_r

        def hops(self, unit, way):
            return 4 if (unit % 2 == 0) == (way > 0) else 3

        def copy(self, unit, source, way, slot):
            ref = self.ref(unit, source)
            return remote(ref, ref, self.send.at[unit, slot], self.recv.at[unit, source], {Y: around(y, way)})

        def hand(self, unit, source):
            ref = self.ref(unit, source)
            return remote(ref, ref, self.hand_s.at[unit, source], self.hand_r.at[unit, source], mate)

        def open(self, unit):
            @pl.when(self.wanted(unit, y))
            def _():
                self.copy(unit, y, 1, y).start()
                self.copy(unit, y, -1, RING).start()

        def step(self, units, hop):
            for unit in units:
                for way in (1, -1):
                    if hop > self.hops(unit, way):
                        continue
                    source = around(y, -way * hop)

                    @pl.when(self.wanted(unit, source))
                    def _(unit=unit, way=way, source=source):
                        self.copy(unit, source, way, source).wait_recv()
                        if hop < self.hops(unit, way):
                            self.copy(unit, source, way, source).start()
                        self.hand(unit, source).start()

        def drain(self, units):
            for unit in units:

                @pl.when(self.wanted(unit, y))
                def _(unit=unit):
                    self.copy(unit, y, 1, y).wait_send()
                    self.copy(unit, y, -1, RING).wait_send()

                for way in (1, -1):
                    for hop in range(1, self.hops(unit, way) + 1):
                        source = around(y, -way * hop)

                        @pl.when(self.wanted(unit, source))
                        def _(unit=unit, way=way, hop=hop, source=source):
                            if hop < self.hops(unit, way):
                                self.copy(unit, source, way, source).wait_send()
                            self.hand(unit, source).wait_send()

        def collect(self, units):
            for unit in units:
                for by in range(1, RING):
                    source = around(y, by)

                    @pl.when(self.wanted(unit, source))
                    def _(unit=unit, source=source):
                        self.hand(unit, source).wait_recv()

    rows_ring = Ring(lambda unit, s: p_ref(s, unit), lambda unit, s: s >= 0, p_send, p_recv, p_hand_send, p_hand_recv)
    slab_ring = Ring(s_ref, s_needed, s_send, s_recv, s_hand_send, s_hand_recv)
    PU, SU = range(2), range(5)

    @pl.when(is_plane)
    def _():
        @pl.when(row < 2)
        def _():
            slabs[row, y] = panel[y, 0:512, :]
            sides[PLANE, row] = rhs[0]
            pair_side.wait_recv()

        pair_piv.wait_recv()

        order = [("L", 0), ("R", 0), ("D", 0)] + [("R", index) for index in range(1, ROUNDS)]
        for at in range(3):
            if order[at][0] == "D":

                @pl.when((row < 2) & (y // 4 == row))
                def _():
                    block = panel[y, pl.ds(pl.multiple_of((y % 4) * 128, 128), 128), :]
                    lane = iota((1, 64), 1)
                    both = [sibling_piv[0:1, :], piv[0:1, :]] if PLANE == 1 else [piv[0:1, :], sibling_piv[0:1, :]]
                    inverses[y] = invert_diagonal(block, jnp.concatenate(both, axis=1))

            relay(*order[at], False)

        def round_of(index, carry):
            relay("R", index, False)

            @pl.when(index == LAG)
            def _():
                relay("L", 0, True)
                relay("D", 0, True)

            @pl.when(index >= LAG)
            def _():
                relay("R", index - LAG, True)

            return carry

        lax.fori_loop(1, ROUNDS, round_of, 0)

        def late_round(index, carry):
            relay("R", index, True)
            return carry

        lax.fori_loop(ROUNDS - LAG, ROUNDS, late_round, 0)
        rows_ring.collect(PU)
        slab_ring.collect(SU)

    @pl.when(is_ridge)
    def _():
        pair_piv.wait_recv()

        @pl.when(row < 2)
        def _():
            sides[RIDGE, row] = rhs[0]

        for unit in PU:
            rows_ring.open(unit)
        for hop in range(1, 5):
            rows_ring.step(PU, hop)
        for unit in range(4):
            kind, tile, tree = UNIT[unit]

            @pl.when(needed(kind, tile, tree, y))
            def _(kind=kind, tile=tile, tree=tree):
                hand_copy(kind, tile, tree, 0).wait_recv()

            slab_ring.open(unit)
        for tile in range(2):

            @pl.when(needed("D", tile, 0, y))
            def _(tile=tile):
                hand_copy("D", tile, 0, 0).wait_recv()
                hand_copy("D", tile, 1, 0).wait_recv()

        slab_ring.open(4)
        for hop in range(1, 5):
            slab_ring.step(SU, hop)

        def take(index, carry):
            for tile in range(2):
                for tree in range(2):
                    root, _, _ = roles(tile, tree)

                    @pl.when(hands("R", root))
                    def _(tile=tile, tree=tree):
                        hand_copy("R", tile, tree, index).wait_recv()

            return carry

        lax.fori_loop(0, ROUNDS, take, 0)

    def lower(tile, top, bottom, left, right):
        return jnp.concatenate(
            [slabs[tile, tile * 4 + j, top * 128 : bottom * 128, :] for j in range(left, right)], axis=1
        )

    def stack(a, c, b):
        zero = jnp.zeros((a.shape[0], b.shape[1]), F32)
        return jnp.concatenate(
            [jnp.concatenate([a, zero], axis=1), jnp.concatenate([c, b], axis=1)], axis=0
        )

    def inverse_of(tile):
        d = [inverses[tile * 4 + j] for j in range(4)]
        c10 = -dot_both(d[1], dot_exact_left(lower(tile, 1, 2, 0, 1), d[0]))
        c32 = -dot_both(d[3], dot_exact_left(lower(tile, 3, 4, 2, 3), d[2]))
        a, b = stack(d[0], c10, d[1]), stack(d[2], c32, d[3])
        c = -dot_both(b, dot_exact_left(lower(tile, 2, 4, 0, 2), a))
        return a, b, c

    a0, b0, c0 = inverse_of(0)
    a1, b1, c1 = inverse_of(1)
    top = sides[core, 0, 0:256, :]
    bottom = sides[core, 0, 256:512, :]
    full[0:256, :] = dot_exact_right(a0, top)
    full[256:512, :] = dot_exact_right(c0, top) + dot_exact_right(b0, bottom)
    low[0:512, :] = full[0:512, :].astype(BF16)
    link = jnp.concatenate([slabs[1, j] for j in range(4)], axis=1)
    rest = sides[core, 1].astype(F32) - dot(link, low[0:512, :])
    full[512:768, :] = dot_both(a1, rest[0:256, :])
    full[768:1024, :] = dot_both(c1, rest[0:256, :]) + dot_both(b1, rest[256:512, :])
    low[512:1024, :] = full[512:1024, :].astype(BF16)

    def put(layer):
        return pltpu.make_async_copy(out.at[layer], out_hbm.at[layer], local_sem.at[3 + layer])

    for layer in range(2):
        for at in range(0, 512, 256):
            rows = slice(layer * 512 + at, layer * 512 + at + 256)
            left = jnp.concatenate([panel[j, rows, :] for j in range(RING)], axis=1)
            out[layer, at : at + 256, :] = rhs[layer, at : at + 256, :].astype(F32) - dot(left, low[...])
        if layer == 0:

            @pl.when(row == 0)
            def _():
                out[0] = full[0:512, :]

            @pl.when(row == 1)
            def _():
                out[0] = full[512:1024, :]

        put(layer).start()

    pair_panel.wait_send()
    pair_piv.wait_send()

    @pl.when((row < 2) & is_ridge)
    def _():
        pair_side.wait_send()

    @pl.when(is_plane)
    def _():
        drain("L", 0)
        drain("D", 0)

        def drain_round(index, carry):
            drain("R", index)
            return carry

        lax.fori_loop(0, ROUNDS, drain_round, 0)

    @pl.when(is_ridge)
    def _():
        rows_ring.drain(PU)
        slab_ring.drain(SU)

    put(0).wait()
    put(1).wait()


def on_device(rhs, panel, pivots):
    dma = pltpu.SemaphoreType.DMA
    slots = ROUNDS + 2
    anywhere = pl.BlockSpec(memory_space=pl.ANY)
    return pl.pallas_call(
        kernel,
        out_shape=jax.ShapeDtypeStruct(rhs.shape, F32),
        in_specs=[anywhere] * 3,
        out_specs=anywhere,
        scratch_shapes=[
            pltpu.VMEM((2, 512, 64), BF16),
            pltpu.VMEM((2, 512, 64), BF16),
            pltpu.VMEM((1, 64), F32),
            pltpu.VMEM((1, 64), F32),
            pltpu.VMEM((2, 512, 512), BF16),
            pltpu.VMEM((RING, 1024, 128), BF16),
            pltpu.VMEM((2, 2, 512, 512), BF16),
            pltpu.VMEM((2, RING, 512, 128), BF16),
            pltpu.VMEM((RING, 128, 128), F32),
            pltpu.VMEM((1024, 512), BF16),
            pltpu.VMEM((1024, 512), F32),
            pltpu.VMEM((2, 512, 512), F32),
            dma((5,)),
            dma((3,)),
            dma((3,)),
            dma((2, 2, 4, slots)),
            dma((2, 2, slots)),
            dma((2, 2, slots)),
            dma((2, 2, slots)),
            dma((2, RING + 1)),
            dma((2, RING)),
            dma((2, RING)),
            dma((2, RING)),
            dma((5, RING + 1)),
            dma((5, RING)),
            dma((5, RING)),
            dma((5, RING)),
        ],
        compiler_params=pltpu.CompilerParams(
            collective_id=0, has_side_effects=True, vmem_limit_bytes=40 * 1024 * 1024
        ),
    )(rhs, panel, pivots.reshape(1, 64))


def solution(mesh):
    torus = Mesh(mesh.devices.reshape(8, 8, 8, 2), (X, Z, Y, CORE))
    return jax.shard_map(
        on_device,
        mesh=torus,
        in_specs=(P(None, (X, Z), (Y, CORE)), P(None, (X, Z), (Y, CORE)), P((Y, CORE))),
        out_specs=P(None, (X, Z), (Y, CORE)),
        check_vma=False,
    )
```

```python
import functools

import jax
import jax.numpy as jnp
from jax import lax
from jax.experimental import pallas as pl
from jax.experimental.pallas import tpu as pltpu
from jax.sharding import Mesh
from jax.sharding import PartitionSpec as P

MESH = pl.DeviceIdType.MESH
F32 = jnp.float32
BF16 = jnp.bfloat16
X, Z, Y, CORE = "row_0", "row_1", "col_0", "col_1"
RING = 8
PLANE, RIDGE = 1, 0
ROUNDS = 8
DEEP = 256 // ROUNDS
LAG = 2
ORDER = 3


def dot(a, b):
    return jnp.dot(a, b, preferred_element_type=F32)


def dot_turned(a, b):
    return lax.dot_general(a, b, (((0,), (0,)), ((), ())), preferred_element_type=F32)


def split(v):
    high = v.astype(BF16)
    return high, (v - high.astype(F32)).astype(BF16)


def dot_exact_left(a, b):
    high, low = split(b)
    return dot(a, high) + dot(a, low)


def dot_exact_right(a, b):
    high, low = split(a)
    return dot(high, b) + dot(low, b)


def dot_both(a, b):
    ah, al = split(a)
    bh, bl = split(b)
    return dot(ah, bh) + (dot(ah, bl) + dot(al, bh))


def iota(shape, dim):
    return lax.broadcasted_iota(jnp.int32, shape, dim)


def invert_diagonal(block, pivots):
    n, base = 128, 32
    rows, cols = iota((n, n), 0), iota((n, n), 1)
    raw = jnp.where(rows > cols, block.astype(F32), 0.0)
    inverse_row = 1.0 / pivots
    inverse_col = jnp.sum(jnp.where(rows == cols, inverse_row, 0.0), axis=1, keepdims=True)
    scaled = raw * inverse_col
    parts = []
    for at in range(0, n, base):
        lower = scaled[at : at + base, :]
        part = (iota((base, n), 0) + at == iota((base, n), 1)).astype(F32)
        for j in range(base - 1):
            part = part - lower[:, at + j : at + j + 1] * part[j : j + 1, :]
        parts.append(part)
    result = jnp.concatenate(parts, axis=0)
    inside = rows // base == cols // base
    result = jnp.where(inside, result, 0.0) * inverse_row
    size = base
    while size < n:
        below = (rows // size) % 2 == 1
        mask = below & (cols // size == rows // size - 1)
        link = jnp.where(mask, raw, 0.0).astype(BF16)
        result = result - dot_both(result, dot_exact_left(link, result))
        size *= 2
    return result


def kernel(
    rhs_hbm, panel_hbm, pivots_hbm, out,
    own, sibling_own, piv, sibling_piv, rhs, panel, sides, slabs, inverses, low, full,
    local_sem, pair_send, pair_recv,
    plane_send, plane_recv, hand_send, hand_recv,
    p_send, p_recv, p_hand_send, p_hand_recv,
    s_send, s_recv, s_hand_send, s_hand_recv,
):
    x, z, y, core = (lax.axis_index(name) for name in (X, Z, Y, CORE))
    row = x * RING + z
    is_plane = core == PLANE
    is_ridge = core == RIDGE

    def around(value, by):
        return lax.rem(value + by + RING, RING)

    def span(value):
        return jnp.minimum(value, RING - value)

    def remote(src, dst, send, recv, where):
        return pltpu.make_async_remote_copy(
            src_ref=src, dst_ref=dst, send_sem=send, recv_sem=recv, device_id=where, device_id_type=MESH
        )

    mate = {CORE: 1 - core}

    take_panel = pltpu.make_async_copy(panel_hbm, own, local_sem.at[0])
    take_piv = pltpu.make_async_copy(pivots_hbm, piv, local_sem.at[1])
    take_rhs = pltpu.make_async_copy(rhs_hbm, rhs, local_sem.at[2])
    take_panel.start()
    take_piv.start()
    take_rhs.start()
    barrier = pltpu.get_barrier_semaphore()
    pl.semaphore_signal(barrier, inc=1, device_id=mate, device_id_type=MESH)

    @pl.when(is_plane)
    def _():
        for by in (1, -1):
            pl.semaphore_signal(barrier, inc=1, device_id={X: around(x, by)}, device_id_type=MESH)
            pl.semaphore_signal(barrier, inc=1, device_id={Z: around(z, by)}, device_id_type=MESH)
        pl.semaphore_wait(barrier, 5)

    @pl.when(is_ridge)
    def _():
        for by in (1, -1):
            pl.semaphore_signal(barrier, inc=1, device_id={Y: around(y, by)}, device_id_type=MESH)
        pl.semaphore_wait(barrier, 3)

    take_panel.wait()
    pair_panel = remote(own, sibling_own, pair_send.at[0], pair_recv.at[0], mate)
    pair_panel.start()
    take_piv.wait()
    pair_piv = remote(piv, sibling_piv, pair_send.at[1], pair_recv.at[1], mate)
    pair_piv.start()
    take_rhs.wait()
    pair_side = remote(rhs.at[0], sides.at[RIDGE, row], pair_send.at[2], pair_recv.at[2], mate)
    pair_inverse = remote(inverses.at[y], inverses.at[y], pair_send.at[3], pair_recv.at[3], mate)

    @pl.when((row < 2) & is_ridge)
    def _():
        pair_side.start()

    pair_panel.wait_recv()
    lane, place = iota((64, 128), 1), iota((64, 128), 0)
    mine = (lane == place + core * 64).astype(BF16)
    theirs = (lane == place + (1 - core) * 64).astype(BF16)
    for layer in range(2):
        chip = (dot_turned(own[layer], mine) + dot_turned(sibling_own[layer], theirs)).astype(BF16)
        panel[y, layer * 512 : (layer + 1) * 512, :] = chip
    pair_piv.wait_recv()

    @pl.when(row < 2)
    def _():
        slabs[row, y] = panel[y, 0:512, :]
        sides[core, row] = rhs[0]

    def needed(kind, tile, tree, at):
        if kind == "R":
            return at >= 0
        if kind == "D":
            return at // 4 == tile
        if tile == 0:
            return (at == 0) if tree == 0 else (at < 3)
        return (at <= 4) if tree == 0 else (at < 7)

    def piece(kind, tile, tree, index, of=None):
        if kind == "R":
            rows = pl.ds(tree * 256 + index * DEEP, DEEP)
            return sides.at[:, tile, rows, :] if of is None else sides.at[of, tile, rows, :]
        if kind == "D":
            return inverses.at[y, tree * 64 : (tree + 1) * 64, :]
        if tile == 0:
            return slabs.at[0, y, 128:256, :] if tree == 0 else slabs.at[0, y, 256:512, :]
        return slabs.at[1, y, 0:256, :] if tree == 0 else slabs.at[1, y, 256:512, :]

    SLOT = {"L": 0, "D": 1, "R": 2}
    first_of = (Z, X)
    second_of = (X, Z)

    def roles(tile, tree):
        to_z = lax.rem(z - tile + RING, RING)
        f, g = (to_z, x) if tree == 0 else (x, to_z)
        root = (f == 0) & (g == 0)
        late = (f == 0) & (g != 0)
        up_first = (g == 0) & (f <= 3)
        down_first = ((g == 0) & ((f == 0) | (f >= 6))) | ((f == 1) & (g != 0))
        up_second = (f != 0) & (g <= 3)
        down_second = (f != 0) & ((g == 0) | (g >= 6))
        depth = span(f) + span(g) + jnp.where(late, 2, 0)
        return root, depth, (up_first, down_first, up_second, down_second)

    def targets(tree):
        at = {X: x, Z: z}
        a, b = first_of[tree], second_of[tree]
        return [{a: around(at[a], 1)}, {a: around(at[a], -1)}, {b: around(at[b], 1)}, {b: around(at[b], -1)}]

    def plane_copy(kind, tile, tree, index, direction):
        ref = piece(kind, tile, tree, index)
        slot = SLOT[kind] + index
        return remote(
            ref, ref, plane_send.at[tile, tree, direction, SLOT[kind]], plane_recv.at[tile, tree, slot],
            targets(tree)[direction],
        )

    def hand_copy(kind, tile, tree, index):
        ref = piece(kind, tile, tree, index, of=RIDGE)
        at = SLOT[kind]
        return remote(ref, ref, hand_send.at[tile, tree, at], hand_recv.at[tile, tree, at], mate)

    def all_rounds(tile, tree, way=None):
        rows = slice(tree * 256, (tree + 1) * 256)
        at = SLOT["R"]
        if way is None:
            ref = sides.at[RIDGE, tile, rows, :]
            return remote(ref, ref, hand_send.at[tile, tree, at], hand_recv.at[tile, tree, at], mate)
        ref = sides.at[:, tile, rows, :]
        return remote(ref, ref, plane_send.at[tile, tree, way, at], plane_recv.at[tile, tree, at], mate)

    def relay(kind, tile, tree, index, role):
        root, _, sends = role

        @pl.when(needed(kind, tile, tree, y))
        def _():
            @pl.when(jnp.logical_not(root))
            def _():
                plane_copy(kind, tile, tree, index, 0).wait_recv()

            for direction in range(4):

                @pl.when(sends[direction])
                def _(direction=direction):
                    plane_copy(kind, tile, tree, index, direction).start()

            @pl.when(jnp.logical_not(root))
            def _():
                hand_copy(kind, tile, tree, index).start()

    PU, SU, DU = 8, 7, 2

    def p_ref(unit, source):
        return panel.at[source, pl.ds(unit * 128, 128), :]

    def s_ref(unit, source):
        if unit < 4:
            return slabs.at[1, source, unit * 128 : (unit + 1) * 128, :]
        if unit < 7:
            return slabs.at[0, source, (unit - 3) * 128 : (unit - 2) * 128, :]
        return inverses.at[source, (unit - 7) * 64 : (unit - 6) * 64, :]

    def s_needed(unit, source):
        if unit < 4:
            return source < unit + 4 if unit else source < 4
        if unit < 7:
            return source < unit - 3
        return source >= 0

    def s_count(unit):
        return (unit + 4) if unit < 4 else (unit - 3) if unit < 7 else RING

    def beside(way):
        return {Y: around(y, way)}

    def p_copy(unit, source, way):
        ref = p_ref(unit, source)
        return remote(ref, ref, p_send, p_recv.at[unit, source], beside(way))

    def p_hand(unit, source):
        ref = p_ref(unit, source)
        return remote(ref, ref, p_hand_send, p_hand_recv, mate)

    def s_copy(unit, source, way, slot):
        ref = s_ref(unit, source)
        return remote(ref, ref, s_send.at[unit, slot], s_recv.at[unit, source], beside(way))

    def s_hand(unit, source):
        ref = s_ref(unit, source)
        return remote(ref, ref, s_hand_send.at[unit, source], s_hand_recv.at[unit], mate)

    def s_open(unit):
        @pl.when(s_needed(unit, y))
        def _():
            s_copy(unit, y, 1, y).start()
            s_copy(unit, y, -1, RING).start()

    def reach(unit, way):
        return 4 if (unit % 2 == 0) == (way > 0) else 3

    def s_step(units, hop):
        for unit in units:
            for way in (1, -1):
                if hop > reach(unit, way):
                    continue
                source = around(y, -way * hop)

                @pl.when(s_needed(unit, source))
                def _(unit=unit, way=way, source=source):
                    s_copy(unit, source, way, source).wait_recv()
                    if hop < reach(unit, way):
                        s_copy(unit, source, way, source).start()
                    s_hand(unit, source).start()

    def s_drain(units, hop):
        for unit in units:
            if hop == 0:

                @pl.when(s_needed(unit, y))
                def _(unit=unit):
                    s_copy(unit, y, 1, y).wait_send()
                    s_copy(unit, y, -1, RING).wait_send()

                continue
            for way in (1, -1):
                if hop > reach(unit, way):
                    continue
                source = around(y, -way * hop)

                @pl.when(s_needed(unit, source))
                def _(unit=unit, way=way, source=source):
                    if hop < reach(unit, way):
                        s_copy(unit, source, way, source).wait_send()
                    s_hand(unit, source).wait_send()

    def s_collect(unit):
        def wait(count):
            if unit < 7:
                ref = slabs.at[1, 0:count, 0:128, :]
            else:
                ref = inverses.at[0:count, 0:64, :]
            remote(ref, ref, s_hand_send.at[unit, 0], s_hand_recv.at[unit], mate).wait_recv()

        count, mine_too = s_count(unit), s_needed(unit, y)
        if count > 1:

            @pl.when(mine_too)
            def _():
                wait(count - 1)

        if count < RING:

            @pl.when(jnp.logical_not(mine_too))
            def _():
                wait(count)

    most = panel.at[0:7]

    @pl.when(is_plane)
    def _():
        @pl.when(row < 2)
        def _():
            pair_side.wait_recv()

        streams = [(tile, tree, roles(tile, tree)) for tile in range(2) for tree in range(2)]
        first = functools.reduce(jnp.minimum, [role[1] for _, _, role in streams])
        last = functools.reduce(jnp.maximum, [role[1] for _, _, role in streams])

        def turn(step, carry):
            for tile, tree, role in streams:
                at = step - LAG * role[1]

                @pl.when(at == 0)
                def _(tile=tile, tree=tree, role=role):
                    relay("L", tile, tree, 0, role)

                @pl.when(at == ORDER)
                def _(tile=tile, tree=tree, role=role):
                    if tree == 0:

                        @pl.when(role[0] & needed("D", tile, tree, y))
                        def _():
                            pair_inverse.wait_recv()

                    relay("D", tile, tree, 0, role)

                @pl.when((at > 0) & (at < ROUNDS + 2) & (at != ORDER))
                def _(tile=tile, tree=tree, role=role, at=at):
                    relay("R", tile, tree, at - jnp.where(at < ORDER, 1, 2), role)

            return carry

        lax.fori_loop(LAG * first, LAG * last + ROUNDS + 2, turn, 0)

        for tile, tree, (root, _, sends) in streams:
            for direction in range(4):

                @pl.when(sends[direction])
                def _(tile=tile, tree=tree, direction=direction):
                    for kind in "LD":

                        @pl.when(needed(kind, tile, tree, y))
                        def _(kind=kind):
                            plane_copy(kind, tile, tree, 0, direction).wait_send()

                    all_rounds(tile, tree, direction).wait_send()

            @pl.when(jnp.logical_not(root))
            def _(tile=tile, tree=tree):
                for kind in "LD":

                    @pl.when(needed(kind, tile, tree, y))
                    def _(kind=kind):
                        hand_copy(kind, tile, tree, 0).wait_send()

                all_rounds(tile, tree).wait_send()

        remote(most, most, p_hand_send, p_hand_recv, mate).wait_recv()
        for unit in range(SU + DU):
            s_collect(unit)

    @pl.when(is_ridge)
    def _():
        def p_open(unit, carry):
            p_copy(unit, y, 1).start()
            p_copy(unit, y, -1).start()
            return carry

        lax.fori_loop(0, PU, p_open, 0)

        @pl.when((row < 2) & (y // 4 == row))
        def _():
            block = panel[y, pl.ds(pl.multiple_of((y % 4) * 128, 128), 128), :]
            both = [sibling_piv[0:1, :], piv[0:1, :]] if PLANE == 0 else [piv[0:1, :], sibling_piv[0:1, :]]
            inverses[y] = invert_diagonal(block, jnp.concatenate(both, axis=1))
            pair_inverse.start()

        for hop in range(1, 5):

            def p_step(unit, carry, hop=hop):
                for way in (1, -1):
                    source = around(y, -way * hop)
                    far = (unit % 2 == 0) if way > 0 else (unit % 2 == 1)

                    def arrive(source=source):
                        p_copy(unit, source, way).wait_recv()
                        p_hand(unit, source).start()

                    if hop < 3:
                        p_copy(unit, source, way).wait_recv()
                        p_copy(unit, source, way).start()
                        p_hand(unit, source).start()
                    elif hop == 3:
                        p_copy(unit, source, way).wait_recv()

                        @pl.when(far)
                        def _(source=source, way=way):
                            p_copy(unit, source, way).start()

                        p_hand(unit, source).start()
                    else:

                        @pl.when(far)
                        def _(source=source, way=way):
                            p_copy(unit, source, way).wait_recv()
                            p_hand(unit, source).start()

                return carry

            lax.fori_loop(0, PU, p_step, 0)

        for tile, tree, units in ((1, 0, (0, 1)), (1, 1, (2, 3)), (0, 1, (5, 6)), (0, 0, (4,))):
            root = roles(tile, tree)[0]

            @pl.when(needed("L", tile, tree, y) & jnp.logical_not(root))
            def _(tile=tile, tree=tree):
                hand_copy("L", tile, tree, 0).wait_recv()

            for unit in units:
                s_open(unit)
        for hop in range(1, 6):
            if hop < 5:
                s_step(range(SU), hop)
            if hop == 1:
                for tree in range(2):
                    for tile in range(2):
                        root = roles(tile, tree)[0]

                        @pl.when(needed("D", tile, tree, y) & jnp.logical_not(root))
                        def _(tile=tile, tree=tree):
                            hand_copy("D", tile, tree, 0).wait_recv()

                    s_open(SU + tree)
            else:
                s_step(range(SU, SU + DU), hop - 1)
            if hop < 5:
                s_drain(range(SU), hop - 1)
            if 1 < hop:
                s_drain(range(SU, SU + DU), hop - 2)
        for tile in range(2):
            for tree in range(2):

                @pl.when(jnp.logical_not(roles(tile, tree)[0]))
                def _(tile=tile, tree=tree):
                    all_rounds(tile, tree).wait_recv()

    def lower(tile, top, bottom, left, right):
        return jnp.concatenate(
            [slabs[tile, tile * 4 + j, top * 128 : bottom * 128, :] for j in range(left, right)], axis=1
        )

    def stack(a, c, b):
        zero = jnp.zeros((a.shape[0], b.shape[1]), F32)
        return jnp.concatenate(
            [jnp.concatenate([a, zero], axis=1), jnp.concatenate([c, b], axis=1)], axis=0
        )

    def inverse_of(tile):
        d = [inverses[tile * 4 + j] for j in range(4)]
        c10 = -dot_both(d[1], dot_exact_left(lower(tile, 1, 2, 0, 1), d[0]))
        c32 = -dot_both(d[3], dot_exact_left(lower(tile, 3, 4, 2, 3), d[2]))
        a, b = stack(d[0], c10, d[1]), stack(d[2], c32, d[3])
        c = -dot_both(b, dot_exact_left(lower(tile, 2, 4, 0, 2), a))
        return a, b, c

    a0, b0, c0 = inverse_of(0)
    a1, b1, c1 = inverse_of(1)
    top = sides[core, 0, 0:256, :]
    bottom = sides[core, 0, 256:512, :]
    full[0:256, :] = dot_exact_right(a0, top)
    full[256:512, :] = dot_exact_right(c0, top) + dot_exact_right(b0, bottom)
    low[0:512, :] = full[0:512, :].astype(BF16)
    link = jnp.concatenate([slabs[1, j] for j in range(4)], axis=1)
    rest = sides[core, 1].astype(F32) - dot(link, low[0:512, :])
    full[512:768, :] = dot_both(a1, rest[0:256, :])
    full[768:1024, :] = dot_both(c1, rest[0:256, :]) + dot_both(b1, rest[256:512, :])
    low[512:1024, :] = full[512:1024, :].astype(BF16)

    for layer in range(2):
        for at in range(0, 512, 256):
            rows = slice(layer * 512 + at, layer * 512 + at + 256)
            left = jnp.concatenate([panel[j, rows, :] for j in range(RING)], axis=1)
            out[layer, at : at + 256, :] = rhs[layer, at : at + 256, :].astype(F32) - dot(left, low[...])

    @pl.when(row == 0)
    def _():
        out[0] = full[0:512, :]

    @pl.when(row == 1)
    def _():
        out[0] = full[512:1024, :]

    pair_panel.wait_send()
    pair_piv.wait_send()

    @pl.when(is_ridge)
    def _():
        @pl.when(row < 2)
        def _():
            pair_side.wait_send()

            @pl.when(y // 4 == row)
            def _():
                pair_inverse.wait_send()

        remote(most, most, p_send, p_hand_recv, mate).wait_send()
        remote(most, most, p_hand_send, p_hand_recv, mate).wait_send()
        s_drain(range(SU), 4)
        s_drain(range(SU, SU + DU), 4)


def on_device(rhs, panel, pivots):
    dma = pltpu.SemaphoreType.DMA
    slots = ROUNDS + 2
    far = pl.BlockSpec(memory_space=pltpu.HBM)
    return pl.pallas_call(
        kernel,
        out_shape=jax.ShapeDtypeStruct(rhs.shape, F32),
        in_specs=[far] * 3,
        out_specs=pl.BlockSpec(memory_space=pltpu.VMEM),
        scratch_shapes=[
            pltpu.VMEM((2, 64, 512), BF16),
            pltpu.VMEM((2, 64, 512), BF16),
            pltpu.VMEM((1, 64), F32),
            pltpu.VMEM((1, 64), F32),
            pltpu.VMEM((2, 512, 512), BF16),
            pltpu.VMEM((RING, 1024, 128), BF16),
            pltpu.VMEM((2, 2, 512, 512), BF16),
            pltpu.VMEM((2, RING, 512, 128), BF16),
            pltpu.VMEM((RING, 128, 128), F32),
            pltpu.VMEM((1024, 512), BF16),
            pltpu.VMEM((1024, 512), F32),
            dma((3,)),
            dma((4,)),
            dma((4,)),
            dma((2, 2, 4, 3)),
            dma((2, 2, slots)),
            dma((2, 2, 3)),
            dma((2, 2, 3)),
            dma,
            dma((8, RING)),
            dma,
            dma,
            dma((9, RING + 1)),
            dma((9, RING)),
            dma((9, RING)),
            dma((9,)),
        ],
        compiler_params=pltpu.CompilerParams(
            collective_id=0, has_side_effects=True, vmem_limit_bytes=40 * 1024 * 1024
        ),
    )(*(pltpu.with_memory_space_constraint(a, pltpu.HBM) for a in (rhs, jnp.swapaxes(panel, 1, 2), pivots.reshape(1, 64))))


def solution(mesh):
    torus = Mesh(mesh.devices.reshape(8, 8, 8, 2), (X, Z, Y, CORE))
    return jax.shard_map(
        on_device,
        mesh=torus,
        in_specs=(P(None, (X, Z), (Y, CORE)), P(None, (X, Z), (Y, CORE)), P((Y, CORE))),
        out_specs=P(None, (X, Z), (Y, CORE)),
        check_vma=False,
    )
```

```python
import functools

import jax
import jax.numpy as jnp
from jax import lax
from jax.experimental import pallas as pl
from jax.experimental.pallas import tpu as pltpu
from jax.sharding import Mesh
from jax.sharding import PartitionSpec as P

MESH = pl.DeviceIdType.MESH
F32 = jnp.float32
BF16 = jnp.bfloat16
X, Z, Y, CORE = "row_0", "row_1", "col_0", "col_1"
RING = 8
PLANE, RIDGE = 1, 0
ROUNDS = 8
DEEP = 256 // ROUNDS
LAG = 2


def dot(a, b):
    return jnp.dot(a, b, preferred_element_type=F32)


def dot_turned(a, b):
    return lax.dot_general(a, b, (((0,), (0,)), ((), ())), preferred_element_type=F32)


def split(v):
    high = v.astype(BF16)
    return high, (v - high.astype(F32)).astype(BF16)


def dot_exact_left(a, b):
    high, low = split(b)
    return dot(a, high) + dot(a, low)


def dot_exact_right(a, b):
    high, low = split(a)
    return dot(high, b) + dot(low, b)


def dot_both(a, b):
    ah, al = split(a)
    bh, bl = split(b)
    return dot(ah, bh) + (dot(ah, bl) + dot(al, bh))


def iota(shape, dim):
    return lax.broadcasted_iota(jnp.int32, shape, dim)


def invert_diagonal(block, pivots):
    n, base = 128, 32
    rows, cols = iota((n, n), 0), iota((n, n), 1)
    raw = jnp.where(rows > cols, block.astype(F32), 0.0)
    inverse_row = 1.0 / pivots
    inverse_col = jnp.sum(jnp.where(rows == cols, inverse_row, 0.0), axis=1, keepdims=True)
    scaled = raw * inverse_col
    parts = []
    for at in range(0, n, base):
        lower = scaled[at : at + base, :]
        part = (iota((base, n), 0) + at == iota((base, n), 1)).astype(F32)
        for j in range(base - 1):
            part = part - lower[:, at + j : at + j + 1] * part[j : j + 1, :]
        parts.append(part)
    result = jnp.concatenate(parts, axis=0)
    inside = rows // base == cols // base
    result = jnp.where(inside, result, 0.0) * inverse_row
    size = base
    while size < n:
        below = (rows // size) % 2 == 1
        mask = below & (cols // size == rows // size - 1)
        link = jnp.where(mask, raw, 0.0).astype(BF16)
        result = result - dot_both(result, dot_exact_left(link, result))
        size *= 2
    return result


def kernel(
    rhs_hbm, panel_hbm, pivots_hbm, out,
    own, sibling_own, piv, sibling_piv, rhs, panel, sides, slabs, inverses, low, full,
    ready, local_sem, pair_send, pair_recv,
    r_send, r_recv, r_hand_send, r_hand_recv,
    l_send, l_recv, l_hand_send, l_hand_recv,
    p_send, p_recv, p_hand_send, p_hand_recv,
    s_out, s_recv, s_hand_recv,
):
    x, z, y, core = (lax.axis_index(name) for name in (X, Z, Y, CORE))
    row = x * RING + z
    is_plane = core == PLANE
    is_ridge = core == RIDGE

    def around(value, by):
        return lax.rem(value + by + RING, RING)

    def span(value):
        return jnp.minimum(value, RING - value)

    def remote(src, dst, send, recv, where):
        return pltpu.make_async_remote_copy(
            src_ref=src, dst_ref=dst, send_sem=send, recv_sem=recv, device_id=where, device_id_type=MESH
        )

    mate = {CORE: 1 - core}

    take_panel = pltpu.make_async_copy(panel_hbm, own, local_sem.at[0])
    take_piv = pltpu.make_async_copy(pivots_hbm, piv, local_sem.at[1])
    take_rhs = pltpu.make_async_copy(rhs_hbm, rhs, local_sem.at[2])
    take_panel.start()
    take_piv.start()
    take_rhs.start()
    barrier = pltpu.get_barrier_semaphore()

    @pl.when(is_ridge)
    def _():
        for by in (1, -1):
            pl.semaphore_signal(barrier, inc=1, device_id={Y: around(y, by)}, device_id_type=MESH)
        pl.semaphore_wait(barrier, 3)
        pl.semaphore_signal(ready, inc=1, device_id=mate, device_id_type=MESH)

    @pl.when(is_plane)
    def _():
        pl.semaphore_signal(barrier, inc=1, device_id=mate, device_id_type=MESH)
        for by in (1, -1):
            pl.semaphore_signal(barrier, inc=1, device_id={X: around(x, by)}, device_id_type=MESH)
            pl.semaphore_signal(barrier, inc=1, device_id={Z: around(z, by)}, device_id_type=MESH)
        pl.semaphore_wait(ready, 1)

    take_panel.wait()
    pair_panel = remote(own, sibling_own, pair_send.at[0], pair_recv.at[0], mate)
    pair_panel.start()
    take_piv.wait()
    pair_piv = remote(piv, sibling_piv, pair_send.at[1], pair_recv.at[1], mate)
    pair_piv.start()
    take_rhs.wait()
    pair_side = remote(rhs.at[0], sides.at[RIDGE, row], pair_send.at[2], pair_recv.at[2], mate)

    @pl.when((row < 2) & is_ridge)
    def _():
        pair_side.start()

    pair_panel.wait_recv()
    lane, place = iota((64, 128), 1), iota((64, 128), 0)
    mine = (lane == place + core * 64).astype(BF16)
    theirs = (lane == place + (1 - core) * 64).astype(BF16)
    for layer in range(2):
        chip = (dot_turned(own[layer], mine) + dot_turned(sibling_own[layer], theirs)).astype(BF16)
        panel[y, layer * 512 : (layer + 1) * 512, :] = chip
    pair_piv.wait_recv()

    @pl.when(row < 2)
    def _():
        slabs[row, y] = panel[y, 0:512, :]
        sides[core, row] = rhs[0]

    BLOCKS = {(0, 0): (), (0, 1): (2, 3, 1, 0), (1, 0): (0, 1), (1, 1): (2, 3)}

    def l_needed(tile, block, at):
        return (at <= block) if tile == 0 else (at <= block + 4)

    first_of = (Z, X)
    second_of = (X, Z)

    def roles(tile, tree):
        to_z = lax.rem(z - tile + RING, RING)
        f, g = (to_z, x) if tree == 0 else (x, to_z)
        root = (f == 0) & (g == 0)
        late = (f == 0) & (g != 0)
        up_first = (g == 0) & (f <= 3)
        down_first = ((g == 0) & ((f == 0) | (f >= 6))) | ((f == 1) & (g != 0))
        up_second = (f != 0) & (g <= 3)
        down_second = (f != 0) & ((g == 0) | (g >= 6))
        depth = span(f) + span(g) + jnp.where(late, 2, 0)
        return root, depth, (up_first, down_first, up_second, down_second)

    def targets(tree):
        at = {X: x, Z: z}
        a, b = first_of[tree], second_of[tree]
        return [{a: around(at[a], 1)}, {a: around(at[a], -1)}, {b: around(at[b], 1)}, {b: around(at[b], -1)}]

    def r_ref(tile, tree, index, of):
        return sides.at[of, tile, pl.ds(tree * 256 + index * DEEP, DEEP), :]

    def r_copy(tile, tree, index, direction):
        ref = r_ref(tile, tree, index, slice(None))
        return remote(ref, ref, r_send.at[tile, tree], r_recv.at[tile, tree, index], targets(tree)[direction])

    def r_hand(tile, tree, index):
        ref = r_ref(tile, tree, index, RIDGE)
        return remote(ref, ref, r_hand_send.at[tile, tree], r_hand_recv.at[tile, tree], mate)

    def r_hand_all(tile, tree):
        ref = sides.at[RIDGE, tile, tree * 256 : (tree + 1) * 256, :]
        return remote(ref, ref, r_hand_send.at[tile, tree], r_hand_recv.at[tile, tree], mate)

    def l_ref(tile, block):
        return slabs.at[tile, y, block * 128 : (block + 1) * 128, :]

    def l_copy(tile, tree, block, direction):
        ref = l_ref(tile, block)
        return remote(ref, ref, l_send.at[tile, block], l_recv.at[tile, block], targets(tree)[direction])

    def l_hand(tile, block):
        ref = l_ref(tile, block)
        return remote(ref, ref, l_hand_send.at[tile, block], l_hand_recv.at[tile, block], mate)

    def relay(copy, hand, role):
        root, _, sends = role

        @pl.when(jnp.logical_not(root))
        def _():
            copy(0).wait_recv()

        for direction in range(4):

            @pl.when(sends[direction])
            def _(direction=direction):
                copy(direction).start()

        @pl.when(jnp.logical_not(root))
        def _():
            hand().start()

    PU, SU, DU = 4, 7, 2

    def p_ref(unit, source):
        return panel.at[source, pl.ds(unit * 256, 256), :]

    def s_ref(unit, source):
        if unit < 4:
            return slabs.at[1, source, unit * 128 : (unit + 1) * 128, :]
        if unit < 7:
            return slabs.at[0, source, (unit - 3) * 128 : (unit - 2) * 128, :]
        return inverses.at[source, (unit - 7) * 64 : (unit - 6) * 64, :]

    def s_needed(unit, source):
        if unit < 4:
            return source < unit + 4
        if unit < 7:
            return source < unit - 3
        return source >= 0

    def s_count(unit):
        return (unit + 4) if unit < 4 else (unit - 3) if unit < 7 else RING

    S_AT = [sum(s_count(before) for before in range(unit)) for unit in range(SU + DU)]

    def beside(way):
        return {Y: around(y, way)}

    def p_copy(unit, source, way):
        ref = p_ref(unit, source)
        return remote(ref, ref, p_send, p_recv.at[unit, source], beside(way))

    def p_hand(unit, source):
        ref = p_ref(unit, source)
        return remote(ref, ref, p_hand_send, p_hand_recv, mate)

    def turn_of(way):
        return 0 if way > 0 else 1

    def s_copy(unit, source, way, hop):
        ref = s_ref(unit, source)
        return remote(ref, ref, s_out.at[unit, turn_of(way), hop % 2], s_recv.at[S_AT[unit] + source], beside(way))

    def s_hand(unit, source, way, hop):
        ref = s_ref(unit, source)
        return remote(ref, ref, s_out.at[unit, turn_of(way), hop % 2], s_hand_recv.at[unit], mate)

    def s_sent(unit, way, hop, copies):
        ref = inverses.at[0, 0 : copies * 64, :] if unit >= SU else slabs.at[1, 0, 0 : copies * 128, :]
        remote(ref, ref, s_out.at[unit, turn_of(way), hop % 2], s_hand_recv.at[unit], mate).wait_send()

    def s_open(unit):
        @pl.when(s_needed(unit, y))
        def _():
            s_copy(unit, y, 1, 0).start()
            s_copy(unit, y, -1, 0).start()
            if unit >= SU:
                s_hand(unit, y, 1, 0).start()

    def reach(unit, way):
        return 4 if (unit % 2 == 0) == (way > 0) else 3

    def s_step(units, hop):
        arrivals = [
            (unit, way, around(y, -way * hop)) for unit in units for way in (1, -1) if hop <= reach(unit, way)
        ]
        for unit, way, source in arrivals:

            @pl.when(s_needed(unit, source))
            def _(unit=unit, way=way, source=source):
                s_copy(unit, source, way, hop).wait_recv()
                if hop < reach(unit, way):
                    s_copy(unit, source, way, hop).start()
                if hop == 4:
                    s_hand(unit, source, way, hop).start()

        if hop < 4:
            for unit, way, source in arrivals:

                @pl.when(s_needed(unit, source))
                def _(unit=unit, way=way, source=source):
                    s_hand(unit, source, way, hop).start()

    def s_drain(units, hop):
        for unit in units:
            for way in (1, -1):
                if hop > reach(unit, way):
                    continue
                source = around(y, -way * hop)

                @pl.when(s_needed(unit, source))
                def _(unit=unit, way=way):
                    if hop == 0:
                        s_sent(unit, way, hop, 2 if unit >= SU and way > 0 else 1)
                    else:
                        s_sent(unit, way, hop, 2 if hop < reach(unit, way) else 1)

    def s_collect(unit):
        def wait(count):
            if unit < 7:
                ref = slabs.at[1, 0:count, 0:128, :]
            else:
                ref = inverses.at[0:count, 0:64, :]
            remote(ref, ref, s_out.at[unit, 0, 0], s_hand_recv.at[unit], mate).wait_recv()

        if unit >= 7:
            wait(RING)
            return
        count, mine_too = s_count(unit), s_needed(unit, y)
        if count > 1:

            @pl.when(mine_too)
            def _():
                wait(count - 1)

        @pl.when(jnp.logical_not(mine_too))
        def _():
            wait(count)

    most = panel.at[0:7]

    @pl.when(is_plane)
    def _():
        pl.semaphore_wait(barrier, 4)

        @pl.when(row < 2)
        def _():
            pair_side.wait_recv()

        streams = [(tile, tree, roles(tile, tree)) for tile in range(2) for tree in range(2)]
        first = functools.reduce(jnp.minimum, [role[1] for _, _, role in streams])
        last = functools.reduce(jnp.maximum, [role[1] for _, _, role in streams])

        def turn(step, carry):
            for tile, tree, role in streams:
                at = step - LAG * role[1]

                @pl.when(at == 0)
                def _(tile=tile, tree=tree, role=role):
                    for block in BLOCKS[tile, tree]:

                        @pl.when(l_needed(tile, block, y))
                        def _(block=block):
                            relay(
                                lambda way: l_copy(tile, tree, block, way), lambda: l_hand(tile, block), role
                            )

                @pl.when((at > 0) & (at <= ROUNDS))
                def _(tile=tile, tree=tree, role=role, at=at):
                    relay(
                        lambda way: r_copy(tile, tree, at - 1, way), lambda: r_hand(tile, tree, at - 1), role
                    )

            return carry

        lax.fori_loop(LAG * first, LAG * last + ROUNDS + 1, turn, 0)

        for tile, tree, (root, _, sends) in streams:
            count = functools.reduce(jnp.add, [way.astype(jnp.int32) for way in sends])
            for copies in range(1, 5):

                @pl.when(count == copies)
                def _(tile=tile, tree=tree, copies=copies):
                    ref = panel.at[0 : 2 * copies]
                    remote(ref, ref, r_send.at[tile, tree], r_recv.at[tile, tree, 0], mate).wait_send()
                    for block in BLOCKS[tile, tree]:

                        @pl.when(l_needed(tile, block, y))
                        def _(block=block):
                            ref = panel.at[0, 0 : copies * 128, :]
                            remote(ref, ref, l_send.at[tile, block], l_recv.at[tile, block], mate).wait_send()

            @pl.when(jnp.logical_not(root))
            def _(tile=tile, tree=tree):
                r_hand_all(tile, tree).wait_send()
                for block in BLOCKS[tile, tree]:

                    @pl.when(l_needed(tile, block, y))
                    def _(block=block):
                        l_hand(tile, block).wait_send()

        remote(most, most, p_hand_send, p_hand_recv, mate).wait_recv()
        for unit in range(SU + DU):
            s_collect(unit)

    @pl.when(is_ridge)
    def _():
        def p_open(unit, carry):
            p_copy(unit, y, 1).start()
            p_copy(unit, y, -1).start()
            return carry

        lax.fori_loop(0, PU, p_open, 0)

        def p_step(hop):
            def step(unit, carry):
                for way in (1, -1):
                    source = around(y, -way * hop)
                    far = (unit % 2 == 0) if way > 0 else (unit % 2 == 1)

                    @pl.when(far | (hop < 4))
                    def _(source=source, way=way, far=far):
                        p_copy(unit, source, way).wait_recv()
                        if hop < 4:

                            @pl.when(far | (hop < 3))
                            def _():
                                p_copy(unit, source, way).start()

                        p_hand(unit, source).start()

                return carry

            lax.fori_loop(0, PU, step, 0)

        near = row == 0
        p_step(1)

        @pl.when(jnp.logical_not(near))
        def _():
            for hop in range(2, 5):
                p_step(hop)

        for tile, tree, opens in ((1, 0, {0: 0, 1: 1}), (1, 1, {2: 2, 3: 3}), (0, 1, {2: 5, 3: 6, 1: 4, 0: None})):
            root = roles(tile, tree)[0]
            for block in BLOCKS[tile, tree]:

                @pl.when(l_needed(tile, block, y) & jnp.logical_not(root))
                def _(tile=tile, block=block):
                    l_hand(tile, block).wait_recv()

                if opens[block] is not None:
                    s_open(opens[block])

        block = slabs[y // 4, y, pl.ds(pl.multiple_of((y % 4) * 128, 128), 128), :]
        both = [sibling_piv[0:1, :], piv[0:1, :]] if PLANE == 0 else [piv[0:1, :], sibling_piv[0:1, :]]
        inverses[y] = invert_diagonal(block, jnp.concatenate(both, axis=1))
        for unit in range(SU, SU + DU):
            s_open(unit)
        for hop in range(1, 5):
            s_step(range(SU), hop)
            s_step(range(SU, SU + DU), hop)
            s_drain(range(SU + DU), hop - 1)
            if hop < 4:

                @pl.when(near)
                def _(hop=hop):
                    p_step(hop + 1)

        for tile in range(2):
            for tree in range(2):

                @pl.when(jnp.logical_not(roles(tile, tree)[0]))
                def _(tile=tile, tree=tree):
                    r_hand_all(tile, tree).wait_recv()

    def lower(tile, top, bottom, left, right):
        return jnp.concatenate(
            [slabs[tile, tile * 4 + j, top * 128 : bottom * 128, :] for j in range(left, right)], axis=1
        )

    def stack(a, c, b):
        zero = jnp.zeros((a.shape[0], b.shape[1]), F32)
        return jnp.concatenate(
            [jnp.concatenate([a, zero], axis=1), jnp.concatenate([c, b], axis=1)], axis=0
        )

    def inverse_of(tile):
        d = [inverses[tile * 4 + j] for j in range(4)]
        c10 = -dot_both(d[1], dot_exact_left(lower(tile, 1, 2, 0, 1), d[0]))
        c32 = -dot_both(d[3], dot_exact_left(lower(tile, 3, 4, 2, 3), d[2]))
        a, b = stack(d[0], c10, d[1]), stack(d[2], c32, d[3])
        c = -dot_both(b, dot_exact_left(lower(tile, 2, 4, 0, 2), a))
        return a, b, c

    a0, b0, c0 = inverse_of(0)
    a1, b1, c1 = inverse_of(1)
    top = sides[core, 0, 0:256, :]
    bottom = sides[core, 0, 256:512, :]
    full[0:256, :] = dot_exact_right(a0, top)
    full[256:512, :] = dot_exact_right(c0, top) + dot_exact_right(b0, bottom)
    low[0:512, :] = full[0:512, :].astype(BF16)
    link = jnp.concatenate([slabs[1, j] for j in range(4)], axis=1)
    rest = sides[core, 1].astype(F32) - dot(link, low[0:512, :])
    full[512:768, :] = dot_both(a1, rest[0:256, :])
    full[768:1024, :] = dot_both(c1, rest[0:256, :]) + dot_both(b1, rest[256:512, :])
    low[512:1024, :] = full[512:1024, :].astype(BF16)

    for layer in range(2):
        for at in range(0, 512, 256):
            rows = slice(layer * 512 + at, layer * 512 + at + 256)
            left = jnp.concatenate([panel[j, rows, :] for j in range(RING)], axis=1)
            out[layer, at : at + 256, :] = rhs[layer, at : at + 256, :].astype(F32) - dot(left, low[...])

    @pl.when(row == 0)
    def _():
        out[0] = full[0:512, :]

    @pl.when(row == 1)
    def _():
        out[0] = full[512:1024, :]

    pair_panel.wait_send()
    pair_piv.wait_send()

    @pl.when(is_ridge)
    def _():
        @pl.when(row < 2)
        def _():
            pair_side.wait_send()

        remote(most, most, p_send, p_hand_recv, mate).wait_send()
        remote(most, most, p_hand_send, p_hand_recv, mate).wait_send()
        s_drain(range(SU + DU), 4)


def on_device(rhs, panel, pivots):
    dma = pltpu.SemaphoreType.DMA
    far = pl.BlockSpec(memory_space=pltpu.HBM)
    return pl.pallas_call(
        kernel,
        out_shape=jax.ShapeDtypeStruct(rhs.shape, F32),
        in_specs=[far] * 3,
        out_specs=pl.BlockSpec(memory_space=pltpu.VMEM),
        scratch_shapes=[
            pltpu.VMEM((2, 64, 512), BF16),
            pltpu.VMEM((2, 64, 512), BF16),
            pltpu.VMEM((1, 64), F32),
            pltpu.VMEM((1, 64), F32),
            pltpu.VMEM((2, 512, 512), BF16),
            pltpu.VMEM((RING, 1024, 128), BF16),
            pltpu.VMEM((2, 2, 512, 512), BF16),
            pltpu.VMEM((2, RING, 512, 128), BF16),
            pltpu.VMEM((RING, 128, 128), F32),
            pltpu.VMEM((1024, 512), BF16),
            pltpu.VMEM((1024, 512), F32),
            pltpu.SemaphoreType.REGULAR,
            dma((3,)),
            dma((3,)),
            dma((3,)),
            dma((2, 2)),
            dma((2, 2, ROUNDS)),
            dma((2, 2)),
            dma((2, 2)),
            dma((2, 4)),
            dma((2, 4)),
            dma((2, 4)),
            dma((2, 4)),
            dma,
            dma((4, RING)),
            dma,
            dma,
            dma((9, 2, 2)),
            dma((44,)),
            dma((9,)),
        ],
        compiler_params=pltpu.CompilerParams(
            collective_id=0, has_side_effects=True, vmem_limit_bytes=40 * 1024 * 1024
        ),
    )(*(pltpu.with_memory_space_constraint(a, pltpu.HBM) for a in (rhs, jnp.swapaxes(panel, 1, 2), pivots.reshape(1, 64))))


def solution(mesh):
    torus = Mesh(mesh.devices.reshape(8, 8, 8, 2), (X, Z, Y, CORE))
    return jax.shard_map(
        on_device,
        mesh=torus,
        in_specs=(P(None, (X, Z), (Y, CORE)), P(None, (X, Z), (Y, CORE)), P((Y, CORE))),
        out_specs=P(None, (X, Z), (Y, CORE)),
        check_vma=False,
    )
```

```python
import functools

import jax
import jax.numpy as jnp
from jax import lax
from jax.experimental import pallas as pl
from jax.experimental.pallas import tpu as pltpu
from jax.sharding import Mesh
from jax.sharding import PartitionSpec as P

MESH = pl.DeviceIdType.MESH
F32 = jnp.float32
BF16 = jnp.bfloat16
X, Z, Y, CORE = "row_0", "row_1", "col_0", "col_1"
RING = 8
PLANE, RIDGE = 1, 0
ROUNDS = 16
DEEP = 256 // ROUNDS
NEAR, FAR = 3, 4


def dot(a, b):
    return jnp.dot(a, b, preferred_element_type=F32)


def dot_turned(a, b):
    return lax.dot_general(a, b, (((0,), (0,)), ((), ())), preferred_element_type=F32)


def split(v):
    high = v.astype(BF16)
    return high, (v - high.astype(F32)).astype(BF16)


def dot_exact_left(a, b):
    high, low = split(b)
    return dot(a, high) + dot(a, low)


def dot_exact_right(a, b):
    high, low = split(a)
    return dot(high, b) + dot(low, b)


def dot_both(a, b):
    ah, al = split(a)
    bh, bl = split(b)
    return dot(ah, bh) + (dot(ah, bl) + dot(al, bh))


def iota(shape, dim):
    return lax.broadcasted_iota(jnp.int32, shape, dim)


def invert_diagonal(block, pivots):
    n, base = 128, 16
    rows, cols = iota((n, n), 0), iota((n, n), 1)
    raw = jnp.where(rows > cols, block.astype(F32), 0.0)
    inverse_row = 1.0 / pivots
    inverse_col = jnp.sum(jnp.where(rows == cols, inverse_row, 0.0), axis=1, keepdims=True)
    scaled = raw * inverse_col
    parts = []
    for at in range(0, n, base):
        lower = scaled[at : at + base, :]
        part = (iota((base, n), 0) + at == iota((base, n), 1)).astype(F32)
        for j in range(base - 1):
            part = part - lower[:, at + j : at + j + 1] * part[j : j + 1, :]
        parts.append(part)
    result = jnp.concatenate(parts, axis=0)
    inside = rows // base == cols // base
    result = jnp.where(inside, result, 0.0) * inverse_row
    size = base
    while size < n:
        below = (rows // size) % 2 == 1
        mask = below & (cols // size == rows // size - 1)
        link = jnp.where(mask, raw, 0.0).astype(BF16)
        result = result - dot_both(result, dot_exact_left(link, result))
        size *= 2
    return result


def kernel(
    rhs_hbm, panel_hbm, pivots_hbm, out,
    own, sibling_own, piv, sibling_piv, rhs, panel, sides, slabs, inverses, low, full,
    ready, local_sem, pair_send, pair_recv,
    r_send, r_recv, r_hand_recv,
    l_send, l_recv, l_hand_recv,
    p_send, p_recv, p_hand_send, p_hand_recv,
    s_out, s_recv, s_hand_recv,
):
    x, z, y, core = (lax.axis_index(name) for name in (X, Z, Y, CORE))
    row = x * RING + z
    is_plane = core == PLANE
    is_ridge = core == RIDGE

    def around(value, by):
        return lax.rem(value + by + RING, RING)

    def span(value):
        return jnp.minimum(value, RING - value)

    def remote(src, dst, send, recv, where):
        return pltpu.make_async_remote_copy(
            src_ref=src, dst_ref=dst, send_sem=send, recv_sem=recv, device_id=where, device_id_type=MESH
        )

    mate = {CORE: 1 - core}

    take_panel = pltpu.make_async_copy(panel_hbm, own, local_sem.at[0])
    take_piv = pltpu.make_async_copy(pivots_hbm, piv, local_sem.at[1])
    take_rhs = pltpu.make_async_copy(rhs_hbm, rhs, local_sem.at[2])
    take_panel.start()
    take_piv.start()
    take_rhs.start()
    barrier = pltpu.get_barrier_semaphore()

    @pl.when(is_ridge)
    def _():
        for by in (1, -1):
            pl.semaphore_signal(barrier, inc=1, device_id={Y: around(y, by)}, device_id_type=MESH)
        pl.semaphore_wait(barrier, 3)
        pl.semaphore_signal(ready, inc=1, device_id=mate, device_id_type=MESH)

    @pl.when(is_plane)
    def _():
        pl.semaphore_signal(barrier, inc=1, device_id=mate, device_id_type=MESH)
        for by in (1, -1):
            pl.semaphore_signal(barrier, inc=1, device_id={X: around(x, by)}, device_id_type=MESH)
            pl.semaphore_signal(barrier, inc=1, device_id={Z: around(z, by)}, device_id_type=MESH)
        pl.semaphore_wait(ready, 1)

    take_panel.wait()
    pair_panel = remote(own, sibling_own, pair_send.at[0], pair_recv.at[0], mate)
    pair_panel.start()
    take_piv.wait()
    pair_piv = remote(piv, sibling_piv, pair_send.at[1], pair_recv.at[1], mate)
    pair_piv.start()
    pair_side = remote(rhs.at[0], sides.at[RIDGE, row], pair_send.at[2], pair_recv.at[2], mate)

    pair_panel.wait_recv()
    lane, place = iota((64, 128), 1), iota((64, 128), 0)
    mine = (lane == place + core * 64).astype(BF16)
    theirs = (lane == place + (1 - core) * 64).astype(BF16)
    for layer in range(2):
        chip = (dot_turned(own[layer], mine) + dot_turned(sibling_own[layer], theirs)).astype(BF16)
        panel[y, layer * 512 : (layer + 1) * 512, :] = chip

    @pl.when(row < 2)
    def _():
        slabs[row, y] = panel[y, 0:512, :]

    @pl.when(is_ridge)
    def _():
        take_rhs.wait()

        @pl.when(row < 2)
        def _():
            pair_side.start()
            sides[RIDGE, row] = rhs[0]

    BLOCKS = {(0, 0): (), (0, 1): (0, 1, 2, 3), (1, 0): (0, 1), (1, 1): (2, 3)}

    def l_needed(tile, block, at):
        return (at <= block) if tile == 0 else (at <= block + 4)

    first_of = (Z, X)
    second_of = (X, Z)

    def roles(tile, tree):
        to_z = lax.rem(z - tile + RING, RING)
        f, g = (to_z, x) if tree == 0 else (x, to_z)
        root = (f == 0) & (g == 0)
        late = (f == 0) & (g != 0)
        up_first = (g == 0) & (f <= 3)
        down_first = ((g == 0) & ((f == 0) | (f >= 6))) | ((f == 1) & (g != 0))
        up_second = (f != 0) & (g <= 3)
        down_second = (f != 0) & ((g == 0) | (g >= 6))
        depth = span(f) + span(g) + jnp.where(late, 2, 0)
        return root, depth, (up_first, down_first, up_second, down_second)

    def targets(tree):
        at = {X: x, Z: z}
        a, b = first_of[tree], second_of[tree]
        return [{a: around(at[a], 1)}, {a: around(at[a], -1)}, {b: around(at[b], 1)}, {b: around(at[b], -1)}]

    def r_ref(tile, tree, index, of):
        return sides.at[of, tile, pl.ds(tree * 256 + index * DEEP, DEEP), :]

    def r_copy(tile, tree, index, direction):
        ref = r_ref(tile, tree, index, slice(None))
        return remote(ref, ref, r_send.at[tile, tree], r_recv.at[tile, tree, index], targets(tree)[direction])

    def r_hand(tile, tree, index):
        ref = r_ref(tile, tree, index, RIDGE)
        return remote(ref, ref, r_send.at[tile, tree], r_hand_recv.at[tile, tree], mate)

    def r_hand_all(tile, tree):
        ref = sides.at[RIDGE, tile, tree * 256 : (tree + 1) * 256, :]
        return remote(ref, ref, r_send.at[tile, tree], r_hand_recv.at[tile, tree], mate)

    def l_ref(tile, block):
        return slabs.at[tile, y, block * 128 : (block + 1) * 128, :]

    def l_copy(tile, tree, block, direction):
        ref = l_ref(tile, block)
        return remote(ref, ref, l_send.at[tile, block], l_recv.at[tile, block], targets(tree)[direction])

    def l_hand(tile, block):
        ref = l_ref(tile, block)
        return remote(ref, ref, l_send.at[tile, block], l_hand_recv.at[tile, block], mate)

    def relay(copy, hand, role):
        root, _, sends = role

        @pl.when(jnp.logical_not(root))
        def _():
            copy(0).wait_recv()

        for direction in range(4):

            @pl.when(sends[direction])
            def _(direction=direction):
                copy(direction).start()

        @pl.when(jnp.logical_not(root))
        def _():
            hand().start()

    PU, SU, DU = 4, 7, 2
    SLABS = ((1, 0, 4), (1, 1, 5), (1, 2, 6), (1, 3, 7), (0, 1, 1), (0, 2, 2), (0, 3, 3))

    def p_ref(unit, source):
        return panel.at[source, pl.ds(unit * 256, 256), :]

    def s_ref(unit, source):
        if unit >= SU:
            return inverses.at[source, (unit - SU) * 64 : (unit - SU + 1) * 64, :]
        tile, block, _ = SLABS[unit]
        return slabs.at[tile, source, block * 128 : (block + 1) * 128, :]

    def s_needed(unit, source):
        return source < s_count(unit)

    def s_count(unit):
        return SLABS[unit][2] if unit < SU else RING

    S_AT = [sum(s_count(before) for before in range(unit)) for unit in range(SU + DU)]

    def beside(way):
        return {Y: around(y, way)}

    def p_copy(unit, source, way):
        ref = p_ref(unit, source)
        return remote(ref, ref, p_send, p_recv.at[unit, source], beside(way))

    def p_hand(unit, source):
        ref = p_ref(unit, source)
        return remote(ref, ref, p_hand_send, p_hand_recv, mate)

    def turn_of(way):
        return 0 if way > 0 else 1

    def s_copy(unit, source, way, hop):
        ref = s_ref(unit, source)
        return remote(ref, ref, s_out.at[unit, turn_of(way), hop % 2], s_recv.at[S_AT[unit] + source], beside(way))

    def s_hand(unit, source, way, hop):
        ref = s_ref(unit, source)
        return remote(ref, ref, s_out.at[unit, turn_of(way), hop % 2], s_hand_recv.at[unit], mate)

    def s_sent(unit, way, hop, copies):
        if unit >= SU:
            ref = inverses.at[0, 0 : copies * 64, :]
        else:
            ref = slabs.at[1, 0, 0 : copies * 128, :]
        remote(ref, ref, s_out.at[unit, turn_of(way), hop % 2], s_hand_recv.at[unit], mate).wait_send()

    def s_open(unit):
        @pl.when(s_needed(unit, y))
        def _():
            s_copy(unit, y, 1, 0).start()
            s_copy(unit, y, -1, 0).start()
            if unit >= SU:
                s_hand(unit, y, 1, 0).start()

    def reach(unit, way):
        return 4 if (unit % 2 == 0) == (way > 0) else 3

    def s_step(units, hop):
        arrivals = [
            (unit, way, around(y, -way * hop)) for unit in units for way in (1, -1) if hop <= reach(unit, way)
        ]
        for unit, way, source in arrivals:

            @pl.when(s_needed(unit, source))
            def _(unit=unit, way=way, source=source):
                s_copy(unit, source, way, hop).wait_recv()
                if hop < reach(unit, way):
                    s_copy(unit, source, way, hop).start()
                if hop == 4:
                    s_hand(unit, source, way, hop).start()

        if hop < 4:
            for unit, way, source in arrivals:

                @pl.when(s_needed(unit, source))
                def _(unit=unit, way=way, source=source):
                    s_hand(unit, source, way, hop).start()

    def s_drain(units, hop):
        for unit in units:
            for way in (1, -1):
                if hop > reach(unit, way):
                    continue
                source = around(y, -way * hop)

                @pl.when(s_needed(unit, source))
                def _(unit=unit, way=way):
                    if hop == 0:
                        s_sent(unit, way, hop, 2 if unit >= SU and way > 0 else 1)
                    else:
                        s_sent(unit, way, hop, 2 if hop < reach(unit, way) else 1)

    def s_collect(unit):
        def wait(count):
            if unit < SU:
                ref = slabs.at[1, 0:count, 0:128, :]
            else:
                ref = inverses.at[0:count, 0:64, :]
            remote(ref, ref, s_out.at[unit, 0, 0], s_hand_recv.at[unit], mate).wait_recv()

        if unit >= SU:
            wait(RING)
            return
        count, mine_too = s_count(unit), s_needed(unit, y)
        if count > 1:

            @pl.when(mine_too)
            def _():
                wait(count - 1)

        @pl.when(jnp.logical_not(mine_too))
        def _():
            wait(count)

    most = panel.at[0:7]

    @pl.when(is_plane)
    def _():
        pl.semaphore_wait(barrier, 4)
        pair_piv.wait_recv()

        streams = [(tile, tree, roles(tile, tree)) for tile in range(2) for tree in range(2)]
        first = functools.reduce(jnp.minimum, [role[1] for _, _, role in streams])
        last = functools.reduce(jnp.maximum, [role[1] for _, _, role in streams])

        def by_count(count, root, sent):
            @pl.when(root)
            def _():
                sent(2, 0)

            for copies in range(4):

                @pl.when((count == copies) & jnp.logical_not(root))
                def _(copies=copies):
                    sent(copies, 1)

        def turn(step, carry):
            for tile, tree, role in streams:
                at = step - NEAR * role[1]
                index = step - FAR * role[1] - 1

                @pl.when(at == 0)
                def _(tile=tile, tree=tree, role=role):
                    for block in BLOCKS[tile, tree]:

                        @pl.when(l_needed(tile, block, y))
                        def _(block=block):
                            relay(
                                lambda way: l_copy(tile, tree, block, way), lambda: l_hand(tile, block), role
                            )

                if BLOCKS[tile, tree]:

                    @pl.when(index == ROUNDS // 2)
                    def _(tile=tile, tree=tree, role=role):
                        def sent(copies, hand):
                            for block in BLOCKS[tile, tree]:

                                @pl.when(l_needed(tile, block, y))
                                def _(block=block):
                                    ref = panel.at[0, 0 : (copies + hand) * 128, :]
                                    remote(ref, ref, l_send.at[tile, block], l_recv.at[tile, block], mate).wait_send()

                        by_count(functools.reduce(jnp.add, [way.astype(jnp.int32) for way in role[2]]), role[0], sent)

                @pl.when((index >= 0) & (index < ROUNDS))
                def _(tile=tile, tree=tree, role=role, index=index):
                    if tree == 0:

                        @pl.when(role[0] & (index == 0))
                        def _():
                            take_rhs.wait()
                            sides[PLANE, row] = rhs[0]
                            pair_side.wait_recv()

                    relay(
                        lambda way: r_copy(tile, tree, index, way), lambda: r_hand(tile, tree, index), role
                    )

            return carry

        lax.fori_loop(NEAR * first, FAR * last + ROUNDS + 1, turn, 0)

        @pl.when(row >= 2)
        def _():
            take_rhs.wait()

        for tile, tree, (root, _, sends) in streams:
            count = functools.reduce(jnp.add, [way.astype(jnp.int32) for way in sends])

            def sent(copies, hand, tile=tile, tree=tree):
                ref = panel.at[0 : 2 * copies + hand]
                remote(ref, ref, r_send.at[tile, tree], r_recv.at[tile, tree, 0], mate).wait_send()

            by_count(count, root, sent)

        remote(most, most, p_hand_send, p_hand_recv, mate).wait_recv()
        for unit in range(SU + DU):
            s_collect(unit)

    @pl.when(is_ridge)
    def _():
        def p_open(unit, carry):
            p_copy(unit, y, 1).start()
            p_copy(unit, y, -1).start()
            return carry

        lax.fori_loop(0, PU, p_open, 0)

        def p_step(hop):
            def step(unit, carry):
                for way in (1, -1):
                    source = around(y, -way * hop)
                    far = (unit % 2 == 0) if way > 0 else (unit % 2 == 1)

                    @pl.when(far | (hop < 4))
                    def _(source=source, way=way, far=far):
                        p_copy(unit, source, way).wait_recv()
                        if hop < 4:

                            @pl.when(far | (hop < 3))
                            def _():
                                p_copy(unit, source, way).start()

                        p_hand(unit, source).start()

                return carry

            lax.fori_loop(0, PU, step, 0)

        tile, block = y // 4, y % 4

        def invert_own():
            @pl.when(row != tile)
            def _():
                ref = slabs.at[tile, y, pl.ds(block * 128, 128), :]
                remote(ref, ref, l_send.at[tile, block], l_hand_recv.at[tile, block], mate).wait_recv()

            diagonal = slabs[tile, y, pl.ds(pl.multiple_of(block * 128, 128), 128), :]
            both = [sibling_piv[0:1, :], piv[0:1, :]] if PLANE == 0 else [piv[0:1, :], sibling_piv[0:1, :]]
            inverses[y] = invert_diagonal(diagonal, jnp.concatenate(both, axis=1))
            for unit in range(SU, SU + DU):
                s_open(unit)

        near = row == 0
        early = near & (tile == 0)
        pair_piv.wait_recv()

        @pl.when(early)
        def _():
            invert_own()

        p_step(1)

        @pl.when(jnp.logical_not(near))
        def _():
            for hop in range(2, 5):
                p_step(hop)

        @pl.when(jnp.logical_not(early))
        def _():
            invert_own()

        for tile, tree, opens in ((1, 0, {0: 0, 1: 1}), (1, 1, {2: 2, 3: 3}), (0, 1, {1: 4, 2: 5, 3: 6})):
            root = roles(tile, tree)[0]
            for block in BLOCKS[tile, tree]:

                @pl.when(l_needed(tile, block, y) & jnp.logical_not(root) & (y != tile * 4 + block))
                def _(tile=tile, block=block):
                    l_hand(tile, block).wait_recv()

                if block in opens:
                    s_open(opens[block])

        @pl.when(near)
        def _():
            p_step(2)

        for hop in range(1, 5):
            s_step(range(SU, SU + DU), hop)
            s_step(range(SU), hop)
            s_drain(range(SU + DU), hop - 1)
            if hop < 3:

                @pl.when(near)
                def _(hop=hop):
                    p_step(hop + 2)

        for tile in range(2):
            for tree in range(2):

                @pl.when(jnp.logical_not(roles(tile, tree)[0]))
                def _(tile=tile, tree=tree):
                    r_hand_all(tile, tree).wait_recv()

    def lower(tile, top, bottom, left, right):
        return jnp.concatenate(
            [slabs[tile, tile * 4 + j, top * 128 : bottom * 128, :] for j in range(left, right)], axis=1
        )

    def stack(a, c, b):
        zero = jnp.zeros((a.shape[0], b.shape[1]), F32)
        return jnp.concatenate(
            [jnp.concatenate([a, zero], axis=1), jnp.concatenate([c, b], axis=1)], axis=0
        )

    def inverse_of(tile):
        d = [inverses[tile * 4 + j] for j in range(4)]
        c10 = -dot_both(d[1], dot_exact_left(lower(tile, 1, 2, 0, 1), d[0]))
        c32 = -dot_both(d[3], dot_exact_left(lower(tile, 3, 4, 2, 3), d[2]))
        a, b = stack(d[0], c10, d[1]), stack(d[2], c32, d[3])
        c = -dot_both(b, dot_exact_left(lower(tile, 2, 4, 0, 2), a))
        return a, b, c

    a0, b0, c0 = inverse_of(0)
    a1, b1, c1 = inverse_of(1)
    top = sides[core, 0, 0:256, :]
    full[0:256, :] = dot_exact_right(a0, top)
    full[256:512, :] = dot_exact_right(jnp.concatenate([c0, b0], axis=1), sides[core, 0])
    low[0:512, :] = full[0:512, :].astype(BF16)
    link = jnp.concatenate([slabs[1, j] for j in range(4)], axis=1)
    rest = sides[core, 1].astype(F32) - dot(link, low[0:512, :])
    full[512:768, :] = dot_both(a1, rest[0:256, :])
    full[768:1024, :] = dot_both(jnp.concatenate([c1, b1], axis=1), rest)
    low[512:1024, :] = full[512:1024, :].astype(BF16)

    for layer in range(2):
        for at in range(0, 512, 256):
            rows = slice(layer * 512 + at, layer * 512 + at + 256)
            left = jnp.concatenate([panel[j, rows, :] for j in range(RING)], axis=1)
            out[layer, at : at + 256, :] = rhs[layer, at : at + 256, :].astype(F32) - dot(left, low[...])

    @pl.when(row == 0)
    def _():
        out[0] = full[0:512, :]

    @pl.when(row == 1)
    def _():
        out[0] = full[512:1024, :]

    pair_panel.wait_send()
    pair_piv.wait_send()

    @pl.when(is_ridge)
    def _():
        @pl.when(row < 2)
        def _():
            pair_side.wait_send()

        remote(most, most, p_send, p_hand_recv, mate).wait_send()
        remote(most, most, p_hand_send, p_hand_recv, mate).wait_send()
        s_drain(range(SU + DU), 4)


def on_device(rhs, panel, pivots):
    dma = pltpu.SemaphoreType.DMA
    far = pl.BlockSpec(memory_space=pltpu.HBM)
    return pl.pallas_call(
        kernel,
        out_shape=jax.ShapeDtypeStruct(rhs.shape, F32),
        in_specs=[far] * 3,
        out_specs=pl.BlockSpec(memory_space=pltpu.VMEM),
        scratch_shapes=[
            pltpu.VMEM((2, 64, 512), BF16),
            pltpu.VMEM((2, 64, 512), BF16),
            pltpu.VMEM((1, 64), F32),
            pltpu.VMEM((1, 64), F32),
            pltpu.VMEM((2, 512, 512), BF16),
            pltpu.VMEM((RING, 1024, 128), BF16),
            pltpu.VMEM((2, 2, 512, 512), BF16),
            pltpu.VMEM((2, RING, 512, 128), BF16),
            pltpu.VMEM((RING, 128, 128), F32),
            pltpu.VMEM((1024, 512), BF16),
            pltpu.VMEM((1024, 512), F32),
            pltpu.SemaphoreType.REGULAR,
            dma((3,)),
            dma((3,)),
            dma((3,)),
            dma((2, 2)),
            dma((2, 2, ROUNDS)),
            dma((2, 2)),
            dma((2, 4)),
            dma((2, 4)),
            dma((2, 4)),
            dma,
            dma((4, RING)),
            dma,
            dma,
            dma((9, 2, 2)),
            dma((44,)),
            dma((9,)),
        ],
        compiler_params=pltpu.CompilerParams(
            collective_id=0, has_side_effects=True, vmem_limit_bytes=40 * 1024 * 1024
        ),
    )(*(pltpu.with_memory_space_constraint(a, pltpu.HBM) for a in (rhs, jnp.swapaxes(panel, 1, 2), pivots.reshape(1, 64))))


def solution(mesh):
    torus = Mesh(mesh.devices.reshape(8, 8, 8, 2), (X, Z, Y, CORE))
    return jax.shard_map(
        on_device,
        mesh=torus,
        in_specs=(P(None, (X, Z), (Y, CORE)), P(None, (X, Z), (Y, CORE)), P((Y, CORE))),
        out_specs=P(None, (X, Z), (Y, CORE)),
        check_vma=False,
    )
```

```python
import functools

import jax
import jax.numpy as jnp
from jax import lax
from jax.experimental import pallas as pl
from jax.experimental.pallas import tpu as pltpu
from jax.sharding import Mesh
from jax.sharding import PartitionSpec as P

MESH = pl.DeviceIdType.MESH
F32 = jnp.float32
BF16 = jnp.bfloat16
X, Z, Y, CORE = "row_0", "row_1", "col_0", "col_1"
RING = 8
PLANE, RIDGE = 1, 0
ROUNDS = 16
DEEP = 256 // ROUNDS
NEAR, FAR = 3, 4


def dot(a, b):
    return jnp.dot(a, b, preferred_element_type=F32)


def dot_turned(a, b):
    return lax.dot_general(a, b, (((0,), (0,)), ((), ())), preferred_element_type=F32)


def split(v):
    high = v.astype(BF16)
    return high, (v - high.astype(F32)).astype(BF16)


def dot_exact_left(a, b):
    high, low = split(b)
    return dot(a, high) + dot(a, low)


def dot_exact_right(a, b):
    high, low = split(a)
    return dot(high, b) + dot(low, b)


def dot_both(a, b):
    ah, al = split(a)
    bh, bl = split(b)
    return dot(ah, bh) + (dot(ah, bl) + dot(al, bh))


def iota(shape, dim):
    return lax.broadcasted_iota(jnp.int32, shape, dim)


def invert_diagonal(block, pivots):
    n, base = 128, 16
    rows, cols = iota((n, n), 0), iota((n, n), 1)
    raw = jnp.where(rows > cols, block.astype(F32), 0.0)
    inverse_row = 1.0 / pivots
    inverse_col = jnp.sum(jnp.where(rows == cols, inverse_row, 0.0), axis=1, keepdims=True)
    scaled = raw * inverse_col
    parts = []
    for at in range(0, n, base):
        lower = scaled[at : at + base, :]
        part = (iota((base, n), 0) + at == iota((base, n), 1)).astype(F32)
        for j in range(base - 1):
            part = part - lower[:, at + j : at + j + 1] * part[j : j + 1, :]
        parts.append(part)
    result = jnp.concatenate(parts, axis=0)
    inside = rows // base == cols // base
    result = jnp.where(inside, result, 0.0) * inverse_row
    size = base
    while size < n:
        below = (rows // size) % 2 == 1
        mask = below & (cols // size == rows // size - 1)
        link = jnp.where(mask, raw, 0.0).astype(BF16)
        result = result - dot_both(result, dot_exact_left(link, result))
        size *= 2
    return result


def kernel(
    rhs_hbm, panel_hbm, pivots_hbm, out,
    own, sibling_own, piv, sibling_piv, rhs, panel, sides, slabs, inverses, low, full,
    ready, local_sem, pair_send, pair_recv,
    r_send, r_recv, r_hand_recv,
    l_send, l_recv, l_hand_recv,
    p_send, p_recv, p_hand_send, p_hand_recv,
    s_out, s_recv, s_hand_recv,
):
    x, z, y, core = (lax.axis_index(name) for name in (X, Z, Y, CORE))
    row = x * RING + z
    is_plane = core == PLANE
    is_ridge = core == RIDGE

    def around(value, by):
        return lax.rem(value + by + RING, RING)

    def span(value):
        return jnp.minimum(value, RING - value)

    def remote(src, dst, send, recv, where):
        return pltpu.make_async_remote_copy(
            src_ref=src, dst_ref=dst, send_sem=send, recv_sem=recv, device_id=where, device_id_type=MESH
        )

    mate = {CORE: 1 - core}

    take_panel = pltpu.make_async_copy(panel_hbm, own, local_sem.at[0])
    take_piv = pltpu.make_async_copy(pivots_hbm, piv, local_sem.at[1])
    take_rhs = pltpu.make_async_copy(rhs_hbm, rhs, local_sem.at[2])
    take_panel.start()
    take_piv.start()
    take_rhs.start()
    barrier = pltpu.get_barrier_semaphore()

    @pl.when(is_ridge)
    def _():
        for by in (1, -1):
            pl.semaphore_signal(barrier, inc=1, device_id={Y: around(y, by)}, device_id_type=MESH)
        pl.semaphore_wait(barrier, 3)
        pl.semaphore_signal(ready, inc=1, device_id=mate, device_id_type=MESH)

    @pl.when(is_plane)
    def _():
        pl.semaphore_signal(barrier, inc=1, device_id=mate, device_id_type=MESH)
        for by in (1, -1):
            pl.semaphore_signal(barrier, inc=1, device_id={X: around(x, by)}, device_id_type=MESH)
            pl.semaphore_signal(barrier, inc=1, device_id={Z: around(z, by)}, device_id_type=MESH)
        pl.semaphore_wait(ready, 1)

    take_panel.wait()
    pair_panel = remote(own, sibling_own, pair_send.at[0], pair_recv.at[0], mate)
    pair_panel.start()
    take_piv.wait()
    pair_piv = remote(piv, sibling_piv, pair_send.at[1], pair_recv.at[1], mate)
    pair_piv.start()
    pair_side = remote(rhs.at[0], sides.at[RIDGE, row], pair_send.at[2], pair_recv.at[2], mate)

    pair_panel.wait_recv()
    lane, place = iota((64, 128), 1), iota((64, 128), 0)
    mine = (lane == place + core * 64).astype(BF16)
    theirs = (lane == place + (1 - core) * 64).astype(BF16)
    for layer in range(2):
        chip = (dot_turned(own[layer], mine) + dot_turned(sibling_own[layer], theirs)).astype(BF16)
        panel[y, layer * 512 : (layer + 1) * 512, :] = chip

    @pl.when(row < 2)
    def _():
        slabs[row, y] = panel[y, 0:512, :]

    @pl.when(is_ridge)
    def _():
        take_rhs.wait()

        @pl.when(row < 2)
        def _():
            pair_side.start()
            sides[RIDGE, row] = rhs[0]

    BLOCKS = {(0, 0): (), (0, 1): (0, 1, 2, 3), (1, 0): (0, 1), (1, 1): (2, 3)}

    def l_needed(tile, block, at):
        return (at <= block) if tile == 0 else (at <= block + 4)

    first_of = (Z, X)
    second_of = (X, Z)

    def roles(tile, tree):
        to_z = lax.rem(z - tile + RING, RING)
        f, g = (to_z, x) if tree == 0 else (x, to_z)
        root = (f == 0) & (g == 0)
        late = (f == 0) & (g != 0)
        up_first = (g == 0) & (f <= 3)
        down_first = ((g == 0) & ((f == 0) | (f >= 6))) | ((f == 1) & (g != 0))
        up_second = (f != 0) & (g <= 3)
        down_second = (f != 0) & ((g == 0) | (g >= 6))
        depth = span(f) + span(g) + jnp.where(late, 2, 0)
        return root, depth, (up_first, down_first, up_second, down_second)

    def targets(tree):
        at = {X: x, Z: z}
        a, b = first_of[tree], second_of[tree]
        return [{a: around(at[a], 1)}, {a: around(at[a], -1)}, {b: around(at[b], 1)}, {b: around(at[b], -1)}]

    def r_ref(tile, tree, index, of):
        return sides.at[of, tile, pl.ds(tree * 256 + index * DEEP, DEEP), :]

    def r_copy(tile, tree, index, direction):
        ref = r_ref(tile, tree, index, slice(None))
        return remote(ref, ref, r_send.at[tile, tree], r_recv.at[tile, tree, index], targets(tree)[direction])

    def r_hand(tile, tree, index):
        ref = r_ref(tile, tree, index, RIDGE)
        return remote(ref, ref, r_send.at[tile, tree], r_hand_recv.at[tile, tree], mate)

    def r_hand_all(tile, tree):
        ref = sides.at[RIDGE, tile, tree * 256 : (tree + 1) * 256, :]
        return remote(ref, ref, r_send.at[tile, tree], r_hand_recv.at[tile, tree], mate)

    def l_ref(tile, block):
        return slabs.at[tile, y, block * 128 : (block + 1) * 128, :]

    def l_copy(tile, tree, block, direction):
        ref = l_ref(tile, block)
        return remote(ref, ref, l_send.at[tile, block], l_recv.at[tile, block], targets(tree)[direction])

    def l_hand(tile, block):
        ref = l_ref(tile, block)
        return remote(ref, ref, l_send.at[tile, block], l_hand_recv.at[tile, block], mate)

    def relay(copy, hand, role):
        root, _, sends = role

        @pl.when(jnp.logical_not(root))
        def _():
            copy(0).wait_recv()

        for direction in range(4):

            @pl.when(sends[direction])
            def _(direction=direction):
                copy(direction).start()

        @pl.when(jnp.logical_not(root))
        def _():
            hand().start()

    PU, SU, DU = 4, 7, 2
    SLABS = ((1, 0, 4), (1, 1, 5), (1, 2, 6), (1, 3, 7), (0, 1, 1), (0, 2, 2), (0, 3, 3))

    def p_ref(unit, source):
        return panel.at[source, pl.ds(unit * 256, 256), :]

    def s_ref(unit, source):
        if unit >= SU:
            return inverses.at[source, (unit - SU) * 64 : (unit - SU + 1) * 64, :]
        tile, block, _ = SLABS[unit]
        return slabs.at[tile, source, block * 128 : (block + 1) * 128, :]

    def s_needed(unit, source):
        return source < s_count(unit)

    def s_count(unit):
        return SLABS[unit][2] if unit < SU else RING

    S_AT = [sum(s_count(before) for before in range(unit)) for unit in range(SU + DU)]

    def beside(way):
        return {Y: around(y, way)}

    def p_copy(unit, source, way):
        ref = p_ref(unit, source)
        return remote(ref, ref, p_send, p_recv.at[unit, source], beside(way))

    def p_hand(unit, source):
        ref = p_ref(unit, source)
        return remote(ref, ref, p_hand_send, p_hand_recv, mate)

    def s_copy(unit, source, way):
        ref = s_ref(unit, source)
        return remote(ref, ref, s_out.at[2 if unit >= SU else 0], s_recv.at[S_AT[unit] + source], beside(way))

    def s_hand(unit, source):
        ref = s_ref(unit, source)
        return remote(ref, ref, s_out.at[2 if unit >= SU else 1], s_hand_recv.at[unit], mate)

    def s_open(unit):
        @pl.when(s_needed(unit, y))
        def _():
            s_copy(unit, y, 1).start()
            s_copy(unit, y, -1).start()
            if unit >= SU:
                s_hand(unit, y).start()

    def reach(unit, way):
        return 4 if (unit % 2 == 0) == (way > 0) else 3

    def s_step(units, hop):
        arrivals = [
            (unit, way, around(y, -way * hop)) for unit in units for way in (1, -1) if hop <= reach(unit, way)
        ]
        for unit, way, source in arrivals:

            @pl.when(s_needed(unit, source))
            def _(unit=unit, way=way, source=source):
                s_copy(unit, source, way).wait_recv()
                if hop < reach(unit, way):
                    s_copy(unit, source, way).start()
                if hop == 4:
                    s_hand(unit, source).start()

        if hop < 4:
            for unit, way, source in arrivals:

                @pl.when(s_needed(unit, source))
                def _(unit=unit, way=way, source=source):
                    s_hand(unit, source).start()

    def sent(count, slot):
        ref = full.at[0 : count * 16, :]
        remote(ref, ref, s_out.at[slot], s_hand_recv.at[0], mate).wait_send()

    def s_drain():
        sent(DU * (RING + RING - 1), 2)
        for at in range(RING):
            copies, hands = 0, 0
            for unit in range(SU):
                for source in range(s_count(unit)):
                    if source == at:
                        copies += 2
                        continue
                    up, down = (at - source) % RING, (source - at) % RING
                    way, hop = (1, up) if up <= reach(unit, 1) else (-1, down)
                    copies += hop < reach(unit, way)
                    hands += 1

            @pl.when(y == at)
            def _(copies=copies, hands=hands):
                sent(copies, 0)
                sent(hands, 1)

    def s_collect(unit):
        def wait(count):
            if unit < SU:
                ref = slabs.at[1, 0:count, 0:128, :]
            else:
                ref = inverses.at[0:count, 0:64, :]
            remote(ref, ref, s_out.at[0], s_hand_recv.at[unit], mate).wait_recv()

        if unit >= SU:
            wait(RING)
            return
        count, mine_too = s_count(unit), s_needed(unit, y)
        if count > 1:

            @pl.when(mine_too)
            def _():
                wait(count - 1)

        @pl.when(jnp.logical_not(mine_too))
        def _():
            wait(count)

    most = panel.at[0:7]

    @pl.when(is_plane)
    def _():
        pl.semaphore_wait(barrier, 4)
        pair_piv.wait_recv()

        streams = [(tile, tree, roles(tile, tree)) for tile in range(2) for tree in range(2)]
        first = functools.reduce(jnp.minimum, [role[1] for _, _, role in streams])
        last = functools.reduce(jnp.maximum, [role[1] for _, _, role in streams])

        def by_count(count, root, sent):
            @pl.when(root)
            def _():
                sent(2, 0)

            for copies in range(4):

                @pl.when((count == copies) & jnp.logical_not(root))
                def _(copies=copies):
                    sent(copies, 1)

        def turn(step, carry):
            for tile, tree, role in streams:
                at = step - NEAR * role[1]
                index = step - FAR * role[1] - 1

                @pl.when(at == 0)
                def _(tile=tile, tree=tree, role=role):
                    for block in BLOCKS[tile, tree]:

                        @pl.when(l_needed(tile, block, y))
                        def _(block=block):
                            relay(
                                lambda way: l_copy(tile, tree, block, way), lambda: l_hand(tile, block), role
                            )

                if BLOCKS[tile, tree]:

                    @pl.when(index == ROUNDS // 2)
                    def _(tile=tile, tree=tree, role=role):
                        def sent(copies, hand):
                            for block in BLOCKS[tile, tree]:

                                @pl.when(l_needed(tile, block, y))
                                def _(block=block):
                                    ref = panel.at[0, 0 : (copies + hand) * 128, :]
                                    remote(ref, ref, l_send.at[tile, block], l_recv.at[tile, block], mate).wait_send()

                        by_count(functools.reduce(jnp.add, [way.astype(jnp.int32) for way in role[2]]), role[0], sent)

                @pl.when((index >= 0) & (index < ROUNDS))
                def _(tile=tile, tree=tree, role=role, index=index):
                    if tree == 0:

                        @pl.when(role[0] & (index == 0))
                        def _():
                            take_rhs.wait()
                            sides[PLANE, row] = rhs[0]
                            pair_side.wait_recv()

                    relay(
                        lambda way: r_copy(tile, tree, index, way), lambda: r_hand(tile, tree, index), role
                    )

            return carry

        lax.fori_loop(NEAR * first, FAR * last + ROUNDS + 1, turn, 0)

        @pl.when(row >= 2)
        def _():
            take_rhs.wait()

        for tile, tree, (root, _, sends) in streams:
            count = functools.reduce(jnp.add, [way.astype(jnp.int32) for way in sends])

            def sent(copies, hand, tile=tile, tree=tree):
                ref = panel.at[0 : 2 * copies + hand]
                remote(ref, ref, r_send.at[tile, tree], r_recv.at[tile, tree, 0], mate).wait_send()

            by_count(count, root, sent)

        remote(most, most, p_hand_send, p_hand_recv, mate).wait_recv()
        for unit in range(SU + DU):
            s_collect(unit)

    @pl.when(is_ridge)
    def _():
        def p_open(unit, carry):
            p_copy(unit, y, 1).start()
            p_copy(unit, y, -1).start()
            return carry

        lax.fori_loop(0, PU, p_open, 0)

        def p_step(hop):
            def step(unit, carry):
                for way in (1, -1):
                    source = around(y, -way * hop)
                    far = (unit % 2 == 0) if way > 0 else (unit % 2 == 1)

                    @pl.when(far | (hop < 4))
                    def _(source=source, way=way, far=far):
                        p_copy(unit, source, way).wait_recv()
                        if hop < 4:

                            @pl.when(far | (hop < 3))
                            def _():
                                p_copy(unit, source, way).start()

                        p_hand(unit, source).start()

                return carry

            lax.fori_loop(0, PU, step, 0)

        tile, block = y // 4, y % 4

        def invert_own():
            @pl.when(row != tile)
            def _():
                ref = slabs.at[tile, y, pl.ds(block * 128, 128), :]
                remote(ref, ref, l_send.at[tile, block], l_hand_recv.at[tile, block], mate).wait_recv()

            diagonal = slabs[tile, y, pl.ds(pl.multiple_of(block * 128, 128), 128), :]
            both = [sibling_piv[0:1, :], piv[0:1, :]] if PLANE == 0 else [piv[0:1, :], sibling_piv[0:1, :]]
            inverses[y] = invert_diagonal(diagonal, jnp.concatenate(both, axis=1))
            for unit in range(SU, SU + DU):
                s_open(unit)

        near = row == 0
        early = near & (tile == 0)
        pair_piv.wait_recv()

        @pl.when(early)
        def _():
            invert_own()

        p_step(1)

        @pl.when(jnp.logical_not(near))
        def _():
            for hop in range(2, 5):
                p_step(hop)

        @pl.when(jnp.logical_not(early))
        def _():
            invert_own()

        for tile, tree, opens in ((1, 0, {0: 0, 1: 1}), (1, 1, {2: 2, 3: 3}), (0, 1, {1: 4, 2: 5, 3: 6})):
            root = roles(tile, tree)[0]
            for block in BLOCKS[tile, tree]:

                @pl.when(l_needed(tile, block, y) & jnp.logical_not(root) & (y != tile * 4 + block))
                def _(tile=tile, block=block):
                    l_hand(tile, block).wait_recv()

                if block in opens:
                    s_open(opens[block])

        @pl.when(near)
        def _():
            p_step(2)

        for hop in range(1, 5):
            s_step(range(SU, SU + DU), hop)
            s_step(range(SU), hop)
            if hop < 3:

                @pl.when(near)
                def _(hop=hop):
                    p_step(hop + 2)

        for tile in range(2):
            for tree in range(2):

                @pl.when(jnp.logical_not(roles(tile, tree)[0]))
                def _(tile=tile, tree=tree):
                    r_hand_all(tile, tree).wait_recv()

    def lower(tile, top, bottom, left, right):
        return jnp.concatenate(
            [slabs[tile, tile * 4 + j, top * 128 : bottom * 128, :] for j in range(left, right)], axis=1
        )

    def stack(a, c, b):
        zero = jnp.zeros((a.shape[0], b.shape[1]), F32)
        return jnp.concatenate(
            [jnp.concatenate([a, zero], axis=1), jnp.concatenate([c, b], axis=1)], axis=0
        )

    def inverse_of(tile):
        d = [inverses[tile * 4 + j] for j in range(4)]
        c10 = -dot_both(d[1], dot_exact_left(lower(tile, 1, 2, 0, 1), d[0]))
        c32 = -dot_both(d[3], dot_exact_left(lower(tile, 3, 4, 2, 3), d[2]))
        a, b = stack(d[0], c10, d[1]), stack(d[2], c32, d[3])
        c = -dot_both(b, dot_exact_left(lower(tile, 2, 4, 0, 2), a))
        return a, b, c

    a0, b0, c0 = inverse_of(0)
    a1, b1, c1 = inverse_of(1)
    top = sides[core, 0, 0:256, :]
    full[0:256, :] = dot_exact_right(a0, top)
    full[256:512, :] = dot_exact_right(jnp.concatenate([c0, b0], axis=1), sides[core, 0])
    low[0:512, :] = full[0:512, :].astype(BF16)
    link = jnp.concatenate([slabs[1, j] for j in range(4)], axis=1)
    rest = sides[core, 1].astype(F32) - dot(link, low[0:512, :])
    full[512:768, :] = dot_both(a1, rest[0:256, :])
    full[768:1024, :] = dot_both(jnp.concatenate([c1, b1], axis=1), rest)
    low[512:1024, :] = full[512:1024, :].astype(BF16)

    for layer in range(2):
        for at in range(0, 512, 256):
            rows = slice(layer * 512 + at, layer * 512 + at + 256)
            left = jnp.concatenate([panel[j, rows, :] for j in range(RING)], axis=1)
            out[layer, at : at + 256, :] = rhs[layer, at : at + 256, :].astype(F32) - dot(left, low[...])

    @pl.when(row == 0)
    def _():
        out[0] = full[0:512, :]

    @pl.when(row == 1)
    def _():
        out[0] = full[512:1024, :]

    pair_panel.wait_send()
    pair_piv.wait_send()

    @pl.when(is_ridge)
    def _():
        @pl.when(row < 2)
        def _():
            pair_side.wait_send()

        remote(most, most, p_send, p_hand_recv, mate).wait_send()
        remote(most, most, p_hand_send, p_hand_recv, mate).wait_send()
        s_drain()


def on_device(rhs, panel, pivots):
    dma = pltpu.SemaphoreType.DMA
    far = pl.BlockSpec(memory_space=pltpu.HBM)
    return pl.pallas_call(
        kernel,
        out_shape=jax.ShapeDtypeStruct(rhs.shape, F32),
        in_specs=[far] * 3,
        out_specs=pl.BlockSpec(memory_space=pltpu.VMEM),
        scratch_shapes=[
            pltpu.VMEM((2, 64, 512), BF16),
            pltpu.VMEM((2, 64, 512), BF16),
            pltpu.VMEM((1, 64), F32),
            pltpu.VMEM((1, 64), F32),
            pltpu.VMEM((2, 512, 512), BF16),
            pltpu.VMEM((RING, 1024, 128), BF16),
            pltpu.VMEM((2, 2, 512, 512), BF16),
            pltpu.VMEM((2, RING, 512, 128), BF16),
            pltpu.VMEM((RING, 128, 128), F32),
            pltpu.VMEM((1024, 512), BF16),
            pltpu.VMEM((1024, 512), F32),
            pltpu.SemaphoreType.REGULAR,
            dma((3,)),
            dma((3,)),
            dma((3,)),
            dma((2, 2)),
            dma((2, 2, ROUNDS)),
            dma((2, 2)),
            dma((2, 4)),
            dma((2, 4)),
            dma((2, 4)),
            dma,
            dma((4, RING)),
            dma,
            dma,
            dma((3,)),
            dma((44,)),
            dma((9,)),
        ],
        compiler_params=pltpu.CompilerParams(
            collective_id=0, has_side_effects=True, vmem_limit_bytes=40 * 1024 * 1024
        ),
    )(*(pltpu.with_memory_space_constraint(a, pltpu.HBM) for a in (rhs, jnp.swapaxes(panel, 1, 2), pivots.reshape(1, 64))))


def solution(mesh):
    torus = Mesh(mesh.devices.reshape(8, 8, 8, 2), (X, Z, Y, CORE))
    return jax.shard_map(
        on_device,
        mesh=torus,
        in_specs=(P(None, (X, Z), (Y, CORE)), P(None, (X, Z), (Y, CORE)), P((Y, CORE))),
        out_specs=P(None, (X, Z), (Y, CORE)),
        check_vma=False,
    )
```

```python
import functools

import jax
import jax.numpy as jnp
from jax import lax
from jax.experimental import pallas as pl
from jax.experimental.pallas import tpu as pltpu
from jax.sharding import Mesh
from jax.sharding import PartitionSpec as P

MESH = pl.DeviceIdType.MESH
F32 = jnp.float32
BF16 = jnp.bfloat16
X, Z, Y, CORE = "row_0", "row_1", "col_0", "col_1"
RING = 8
PLANE, RIDGE = 1, 0
ROUNDS = 16
DEEP = 256 // ROUNDS
NEAR, FAR = 3, 4


def dot(a, b):
    return jnp.dot(a, b, preferred_element_type=F32)


def dot_turned(a, b):
    return lax.dot_general(a, b, (((0,), (0,)), ((), ())), preferred_element_type=F32)


def split(v):
    high = v.astype(BF16)
    return high, (v - high.astype(F32)).astype(BF16)


def dot_exact_left(a, b):
    high, low = split(b)
    return dot(a, high) + dot(a, low)


def dot_exact_right(a, b):
    high, low = split(a)
    return dot(high, b) + dot(low, b)


def dot_both(a, b):
    ah, al = split(a)
    bh, bl = split(b)
    return dot(ah, bh) + (dot(ah, bl) + dot(al, bh))


def iota(shape, dim):
    return lax.broadcasted_iota(jnp.int32, shape, dim)


def invert_diagonal(block, pivots):
    n, base = 128, 16
    rows, cols = iota((n, n), 0), iota((n, n), 1)
    raw = jnp.where(rows > cols, block.astype(F32), 0.0)
    inverse_row = 1.0 / pivots
    inverse_col = jnp.sum(jnp.where(rows == cols, inverse_row, 0.0), axis=1, keepdims=True)
    scaled = raw * inverse_col
    parts = []
    for at in range(0, n, base):
        lower = scaled[at : at + base, :]
        part = (iota((base, n), 0) + at == iota((base, n), 1)).astype(F32)
        for j in range(base - 1):
            part = part - lower[:, at + j : at + j + 1] * part[j : j + 1, :]
        parts.append(part)
    result = jnp.concatenate(parts, axis=0)
    inside = rows // base == cols // base
    result = jnp.where(inside, result, 0.0) * inverse_row
    size = base
    while size < n:
        below = (rows // size) % 2 == 1
        mask = below & (cols // size == rows // size - 1)
        link = jnp.where(mask, raw, 0.0).astype(BF16)
        result = result - dot_both(result, dot_exact_left(link, result))
        size *= 2
    return result


def kernel(
    rhs_hbm, panel_hbm, pivots_hbm, out,
    own, sibling_own, piv, sibling_piv, rhs, panel, sides, slabs, inverses, low, full,
    ready, local_sem, pair_send, pair_recv,
    r_send, r_recv, r_hand_recv,
    l_send, l_recv, l_hand_recv,
    p_send, p_recv, p_hand_send, p_hand_recv,
    s_out, s_recv, s_hand_recv,
):
    x, z, y, core = (lax.axis_index(name) for name in (X, Z, Y, CORE))
    row = x * RING + z
    is_plane = core == PLANE
    is_ridge = core == RIDGE

    def around(value, by):
        return lax.rem(value + by + RING, RING)

    def span(value):
        return jnp.minimum(value, RING - value)

    def remote(src, dst, send, recv, where):
        return pltpu.make_async_remote_copy(
            src_ref=src, dst_ref=dst, send_sem=send, recv_sem=recv, device_id=where, device_id_type=MESH
        )

    mate = {CORE: 1 - core}

    take_panel = pltpu.make_async_copy(panel_hbm, own, local_sem.at[0])
    take_piv = pltpu.make_async_copy(pivots_hbm, piv, local_sem.at[1])
    take_rhs = pltpu.make_async_copy(rhs_hbm, rhs, local_sem.at[2])
    take_panel.start()
    take_piv.start()
    take_rhs.start()
    barrier = pltpu.get_barrier_semaphore()

    @pl.when(is_ridge)
    def _():
        for by in (1, -1):
            pl.semaphore_signal(barrier, inc=1, device_id={Y: around(y, by)}, device_id_type=MESH)
        pl.semaphore_wait(barrier, 5)
        pl.semaphore_signal(ready, inc=1, device_id=mate, device_id_type=MESH)

    @pl.when(is_plane)
    def _():
        pl.semaphore_signal(barrier, inc=1, device_id=mate, device_id_type=MESH)
        for by in (1, -1):
            pl.semaphore_signal(barrier, inc=1, device_id={X: around(x, by)}, device_id_type=MESH)
            pl.semaphore_signal(barrier, inc=1, device_id={Z: around(z, by)}, device_id_type=MESH)
            pl.semaphore_signal(barrier, inc=1, device_id={Y: around(y, by), CORE: RIDGE}, device_id_type=MESH)
        pl.semaphore_wait(ready, 1)

    take_panel.wait()
    pair_panel = remote(own, sibling_own, pair_send.at[0], pair_recv.at[0], mate)
    pair_panel.start()
    take_piv.wait()
    pair_piv = remote(piv, sibling_piv, pair_send.at[1], pair_recv.at[1], mate)
    pair_piv.start()
    pair_side = remote(rhs.at[0], sides.at[RIDGE, row], pair_send.at[2], pair_recv.at[2], mate)

    pair_panel.wait_recv()
    lane, place = iota((64, 128), 1), iota((64, 128), 0)
    mine = (lane == place + core * 64).astype(BF16)
    theirs = (lane == place + (1 - core) * 64).astype(BF16)
    for layer in range(2):
        chip = (dot_turned(own[layer], mine) + dot_turned(sibling_own[layer], theirs)).astype(BF16)
        panel[y, layer * 512 : (layer + 1) * 512, :] = chip

    @pl.when(row < 2)
    def _():
        slabs[row, y] = panel[y, 0:512, :]

    @pl.when(is_ridge)
    def _():
        take_rhs.wait()

        @pl.when(row < 2)
        def _():
            pair_side.start()
            sides[RIDGE, row] = rhs[0]

    BLOCKS = {(0, 0): (), (0, 1): (0, 1, 2, 3), (1, 0): (0, 1), (1, 1): (2, 3)}

    def l_needed(tile, block, at):
        return (at <= block) if tile == 0 else (at <= block + 4)

    first_of = (Z, X)
    second_of = (X, Z)

    def roles(tile, tree):
        to_z = lax.rem(z - tile + RING, RING)
        f, g = (to_z, x) if tree == 0 else (x, to_z)
        root = (f == 0) & (g == 0)
        late = (f == 0) & (g != 0)
        up_first = (g == 0) & (f <= 3)
        down_first = ((g == 0) & ((f == 0) | (f >= 6))) | ((f == 1) & (g != 0))
        up_second = (f != 0) & (g <= 3)
        down_second = (f != 0) & ((g == 0) | (g >= 6))
        depth = span(f) + span(g) + jnp.where(late, 2, 0)
        return root, depth, (up_first, down_first, up_second, down_second)

    def targets(tree):
        at = {X: x, Z: z}
        a, b = first_of[tree], second_of[tree]
        return [{a: around(at[a], 1)}, {a: around(at[a], -1)}, {b: around(at[b], 1)}, {b: around(at[b], -1)}]

    def r_ref(tile, tree, index, of):
        return sides.at[of, tile, pl.ds(tree * 256 + index * DEEP, DEEP), :]

    def r_copy(tile, tree, index, direction):
        ref = r_ref(tile, tree, index, slice(None))
        return remote(ref, ref, r_send.at[tile, tree], r_recv.at[tile, tree, index], targets(tree)[direction])

    def r_hand(tile, tree, index):
        ref = r_ref(tile, tree, index, RIDGE)
        return remote(ref, ref, r_send.at[tile, tree], r_hand_recv.at[tile, tree], mate)

    def r_hand_all(tile, tree):
        ref = sides.at[RIDGE, tile, tree * 256 : (tree + 1) * 256, :]
        return remote(ref, ref, r_send.at[tile, tree], r_hand_recv.at[tile, tree], mate)

    def l_ref(tile, block):
        return slabs.at[tile, y, block * 128 : (block + 1) * 128, :]

    def l_copy(tile, tree, block, direction):
        ref = l_ref(tile, block)
        return remote(ref, ref, l_send.at[tile, block], l_recv.at[tile, block], targets(tree)[direction])

    def l_hand(tile, block):
        ref = l_ref(tile, block)
        return remote(ref, ref, l_send.at[tile, block], l_hand_recv.at[tile, block], mate)

    def relay(copy, hand, role):
        root, _, sends = role

        @pl.when(jnp.logical_not(root))
        def _():
            copy(0).wait_recv()

        for direction in range(4):

            @pl.when(sends[direction])
            def _(direction=direction):
                copy(direction).start()

        @pl.when(jnp.logical_not(root))
        def _():
            hand().start()

    PU, SU, DU = 4, 7, 2
    SLABS = ((1, 0, 4), (1, 1, 5), (1, 2, 6), (1, 3, 7), (0, 1, 1), (0, 2, 2), (0, 3, 3))

    def p_ref(unit, source):
        return panel.at[source, pl.ds(unit * 256, 256), :]

    def s_ref(unit, source):
        if unit >= SU:
            return inverses.at[source, (unit - SU) * 64 : (unit - SU + 1) * 64, :]
        tile, block, _ = SLABS[unit]
        return slabs.at[tile, source, block * 128 : (block + 1) * 128, :]

    def s_needed(unit, source):
        return source < s_count(unit)

    def s_count(unit):
        return SLABS[unit][2] if unit < SU else RING

    S_AT = [sum(s_count(before) for before in range(unit)) for unit in range(SU + DU)]

    def beside(way):
        return {Y: around(y, way)}

    def p_copy(unit, source, way):
        ref = p_ref(unit, source)
        return remote(ref, ref, p_send, p_recv.at[unit, source], beside(way))

    def p_hand(unit, source):
        ref = p_ref(unit, source)
        return remote(ref, ref, p_hand_send, p_hand_recv, mate)

    def s_copy(unit, source, way):
        ref = s_ref(unit, source)
        return remote(ref, ref, s_out.at[2 if unit >= SU else 0], s_recv.at[S_AT[unit] + source], beside(way))

    def s_hand(unit, source):
        ref = s_ref(unit, source)
        return remote(ref, ref, s_out.at[2 if unit >= SU else 1], s_hand_recv.at[unit], mate)

    def s_across(unit, source, way):
        ref = s_ref(unit, source)
        where = {Y: around(y, way), CORE: PLANE}
        return remote(ref, ref, s_out.at[2 if unit >= SU else 0], s_hand_recv.at[unit], where)

    def s_open(unit):
        @pl.when(s_needed(unit, y))
        def _():
            s_copy(unit, y, 1).start()
            s_copy(unit, y, -1).start()
            if unit >= SU:
                s_hand(unit, y).start()

    def reach(unit, way):
        return 4 if (unit % 2 == 0) == (way > 0) else 3

    def s_step(units, hop):
        arrivals = [
            (unit, way, around(y, -way * hop)) for unit in units for way in (1, -1) if hop <= reach(unit, way)
        ]
        for unit, way, source in arrivals:

            @pl.when(s_needed(unit, source))
            def _(unit=unit, way=way, source=source):
                s_copy(unit, source, way).wait_recv()
                if hop < reach(unit, way):
                    s_copy(unit, source, way).start()
                    if hop + 1 == reach(unit, way):
                        s_across(unit, source, way).start()

        for unit, way, source in arrivals:
            if hop < reach(unit, way):

                @pl.when(s_needed(unit, source))
                def _(unit=unit, source=source):
                    s_hand(unit, source).start()

    def sent(count, slot):
        ref = full.at[0 : count * 16, :]
        remote(ref, ref, s_out.at[slot], s_hand_recv.at[0], mate).wait_send()

    def s_drain():
        sent(DU * (RING + RING - 1), 2)
        for at in range(RING):
            copies, hands = 0, 0
            for unit in range(SU):
                for source in range(s_count(unit)):
                    if source == at:
                        copies += 2
                        continue
                    up, down = (at - source) % RING, (source - at) % RING
                    way, hop = (1, up) if up <= reach(unit, 1) else (-1, down)
                    copies += (hop < reach(unit, way)) + (hop + 1 == reach(unit, way))
                    hands += hop < reach(unit, way)

            @pl.when(y == at)
            def _(copies=copies, hands=hands):
                sent(copies, 0)
                sent(hands, 1)

    def s_collect(unit):
        def wait(count):
            if unit < SU:
                ref = slabs.at[1, 0:count, 0:128, :]
            else:
                ref = inverses.at[0:count, 0:64, :]
            remote(ref, ref, s_out.at[0], s_hand_recv.at[unit], mate).wait_recv()

        if unit >= SU:
            wait(RING)
            return
        count, mine_too = s_count(unit), s_needed(unit, y)
        if count > 1:

            @pl.when(mine_too)
            def _():
                wait(count - 1)

        @pl.when(jnp.logical_not(mine_too))
        def _():
            wait(count)

    most = panel.at[0:7]

    @pl.when(is_plane)
    def _():
        pl.semaphore_wait(barrier, 4)
        pair_piv.wait_recv()

        streams = [(tile, tree, roles(tile, tree)) for tile in range(2) for tree in range(2)]
        first = functools.reduce(jnp.minimum, [role[1] for _, _, role in streams])
        last = functools.reduce(jnp.maximum, [role[1] for _, _, role in streams])

        def by_count(count, root, sent):
            @pl.when(root)
            def _():
                sent(2, 0)

            for copies in range(4):

                @pl.when((count == copies) & jnp.logical_not(root))
                def _(copies=copies):
                    sent(copies, 1)

        def turn(step, carry):
            for tile, tree, role in streams:
                at = step - NEAR * role[1]
                index = step - FAR * role[1] - 1

                @pl.when(at == 0)
                def _(tile=tile, tree=tree, role=role):
                    for block in BLOCKS[tile, tree]:

                        @pl.when(l_needed(tile, block, y))
                        def _(block=block):
                            relay(
                                lambda way: l_copy(tile, tree, block, way), lambda: l_hand(tile, block), role
                            )

                if BLOCKS[tile, tree]:

                    @pl.when(index == ROUNDS // 2)
                    def _(tile=tile, tree=tree, role=role):
                        def sent(copies, hand):
                            for block in BLOCKS[tile, tree]:

                                @pl.when(l_needed(tile, block, y))
                                def _(block=block):
                                    ref = panel.at[0, 0 : (copies + hand) * 128, :]
                                    remote(ref, ref, l_send.at[tile, block], l_recv.at[tile, block], mate).wait_send()

                        by_count(functools.reduce(jnp.add, [way.astype(jnp.int32) for way in role[2]]), role[0], sent)

                @pl.when((index >= 0) & (index < ROUNDS))
                def _(tile=tile, tree=tree, role=role, index=index):
                    if tree == 0:

                        @pl.when(role[0] & (index == 0))
                        def _():
                            take_rhs.wait()
                            sides[PLANE, row] = rhs[0]
                            pair_side.wait_recv()

                    relay(
                        lambda way: r_copy(tile, tree, index, way), lambda: r_hand(tile, tree, index), role
                    )

            return carry

        lax.fori_loop(NEAR * first, FAR * last + ROUNDS + 1, turn, 0)

        @pl.when(row >= 2)
        def _():
            take_rhs.wait()

        for tile, tree, (root, _, sends) in streams:
            count = functools.reduce(jnp.add, [way.astype(jnp.int32) for way in sends])

            def sent(copies, hand, tile=tile, tree=tree):
                ref = panel.at[0 : 2 * copies + hand]
                remote(ref, ref, r_send.at[tile, tree], r_recv.at[tile, tree, 0], mate).wait_send()

            by_count(count, root, sent)

        remote(most, most, p_hand_send, p_hand_recv, mate).wait_recv()
        for unit in range(SU + DU):
            s_collect(unit)

    @pl.when(is_ridge)
    def _():
        def p_open(unit, carry):
            p_copy(unit, y, 1).start()
            p_copy(unit, y, -1).start()
            return carry

        lax.fori_loop(0, PU, p_open, 0)

        def p_step(hop):
            def step(unit, carry):
                for way in (1, -1):
                    source = around(y, -way * hop)
                    far = (unit % 2 == 0) if way > 0 else (unit % 2 == 1)

                    @pl.when(far | (hop < 4))
                    def _(source=source, way=way, far=far):
                        p_copy(unit, source, way).wait_recv()
                        if hop < 4:

                            @pl.when(far | (hop < 3))
                            def _():
                                p_copy(unit, source, way).start()

                        p_hand(unit, source).start()

                return carry

            lax.fori_loop(0, PU, step, 0)

        tile, block = y // 4, y % 4

        def invert_own():
            @pl.when(row != tile)
            def _():
                ref = slabs.at[tile, y, pl.ds(block * 128, 128), :]
                remote(ref, ref, l_send.at[tile, block], l_hand_recv.at[tile, block], mate).wait_recv()

            diagonal = slabs[tile, y, pl.ds(pl.multiple_of(block * 128, 128), 128), :]
            both = [sibling_piv[0:1, :], piv[0:1, :]] if PLANE == 0 else [piv[0:1, :], sibling_piv[0:1, :]]
            inverses[y] = invert_diagonal(diagonal, jnp.concatenate(both, axis=1))
            for unit in range(SU, SU + DU):
                s_open(unit)

        near = row == 0
        early = near & (tile == 0)
        pair_piv.wait_recv()

        @pl.when(early)
        def _():
            invert_own()

        p_step(1)

        @pl.when(jnp.logical_not(near))
        def _():
            for hop in range(2, 5):
                p_step(hop)

        @pl.when(jnp.logical_not(early))
        def _():
            invert_own()

        for tile, tree, opens in ((1, 0, {0: 0, 1: 1}), (1, 1, {2: 2, 3: 3}), (0, 1, {1: 4, 2: 5, 3: 6})):
            root = roles(tile, tree)[0]
            for block in BLOCKS[tile, tree]:

                @pl.when(l_needed(tile, block, y) & jnp.logical_not(root) & (y != tile * 4 + block))
                def _(tile=tile, block=block):
                    l_hand(tile, block).wait_recv()

                if block in opens:
                    s_open(opens[block])

        @pl.when(near)
        def _():
            p_step(2)

        for hop in range(1, 5):
            s_step(range(SU, SU + DU), hop)
            s_step(range(SU), hop)
            if hop < 3:

                @pl.when(near)
                def _(hop=hop):
                    p_step(hop + 2)

        for tile in range(2):
            for tree in range(2):

                @pl.when(jnp.logical_not(roles(tile, tree)[0]))
                def _(tile=tile, tree=tree):
                    r_hand_all(tile, tree).wait_recv()

    def lower(tile, top, bottom, left, right):
        return jnp.concatenate(
            [slabs[tile, tile * 4 + j, top * 128 : bottom * 128, :] for j in range(left, right)], axis=1
        )

    def stack(a, c, b):
        zero = jnp.zeros((a.shape[0], b.shape[1]), F32)
        return jnp.concatenate(
            [jnp.concatenate([a, zero], axis=1), jnp.concatenate([c, b], axis=1)], axis=0
        )

    def inverse_of(tile):
        d = [inverses[tile * 4 + j] for j in range(4)]
        c10 = -dot_both(d[1], dot_exact_left(lower(tile, 1, 2, 0, 1), d[0]))
        c32 = -dot_both(d[3], dot_exact_left(lower(tile, 3, 4, 2, 3), d[2]))
        a, b = stack(d[0], c10, d[1]), stack(d[2], c32, d[3])
        c = -dot_both(b, dot_exact_left(lower(tile, 2, 4, 0, 2), a))
        return a, b, c

    a0, b0, c0 = inverse_of(0)
    a1, b1, c1 = inverse_of(1)
    top = sides[core, 0, 0:256, :]
    full[0:256, :] = dot_exact_right(a0, top)
    full[256:512, :] = dot_exact_right(jnp.concatenate([c0, b0], axis=1), sides[core, 0])
    low[0:512, :] = full[0:512, :].astype(BF16)
    link = jnp.concatenate([slabs[1, j] for j in range(4)], axis=1)
    rest = sides[core, 1].astype(F32) - dot(link, low[0:512, :])
    full[512:768, :] = dot_both(a1, rest[0:256, :])
    full[768:1024, :] = dot_both(jnp.concatenate([c1, b1], axis=1), rest)
    low[512:1024, :] = full[512:1024, :].astype(BF16)

    for layer in range(2):
        for at in range(0, 512, 256):
            rows = slice(layer * 512 + at, layer * 512 + at + 256)
            left = jnp.concatenate([panel[j, rows, :] for j in range(RING)], axis=1)
            out[layer, at : at + 256, :] = rhs[layer, at : at + 256, :].astype(F32) - dot(left, low[...])

    @pl.when(row == 0)
    def _():
        out[0] = full[0:512, :]

    @pl.when(row == 1)
    def _():
        out[0] = full[512:1024, :]

    pair_panel.wait_send()
    pair_piv.wait_send()

    @pl.when(is_ridge)
    def _():
        @pl.when(row < 2)
        def _():
            pair_side.wait_send()

        remote(most, most, p_send, p_hand_recv, mate).wait_send()
        remote(most, most, p_hand_send, p_hand_recv, mate).wait_send()
        s_drain()


def on_device(rhs, panel, pivots):
    dma = pltpu.SemaphoreType.DMA
    far = pl.BlockSpec(memory_space=pltpu.HBM)
    return pl.pallas_call(
        kernel,
        out_shape=jax.ShapeDtypeStruct(rhs.shape, F32),
        in_specs=[far] * 3,
        out_specs=pl.BlockSpec(memory_space=pltpu.VMEM),
        scratch_shapes=[
            pltpu.VMEM((2, 64, 512), BF16),
            pltpu.VMEM((2, 64, 512), BF16),
            pltpu.VMEM((1, 64), F32),
            pltpu.VMEM((1, 64), F32),
            pltpu.VMEM((2, 512, 512), BF16),
            pltpu.VMEM((RING, 1024, 128), BF16),
            pltpu.VMEM((2, 2, 512, 512), BF16),
            pltpu.VMEM((2, RING, 512, 128), BF16),
            pltpu.VMEM((RING, 128, 128), F32),
            pltpu.VMEM((1024, 512), BF16),
            pltpu.VMEM((1024, 512), F32),
            pltpu.SemaphoreType.REGULAR,
            dma((3,)),
            dma((3,)),
            dma((3,)),
            dma((2, 2)),
            dma((2, 2, ROUNDS)),
            dma((2, 2)),
            dma((2, 4)),
            dma((2, 4)),
            dma((2, 4)),
            dma,
            dma((4, RING)),
            dma,
            dma,
            dma((3,)),
            dma((44,)),
            dma((9,)),
        ],
        compiler_params=pltpu.CompilerParams(
            collective_id=0, has_side_effects=True, vmem_limit_bytes=40 * 1024 * 1024
        ),
    )(*(pltpu.with_memory_space_constraint(a, pltpu.HBM) for a in (rhs, jnp.swapaxes(panel, 1, 2), pivots.reshape(1, 64))))


def solution(mesh):
    torus = Mesh(mesh.devices.reshape(8, 8, 8, 2), (X, Z, Y, CORE))
    return jax.shard_map(
        on_device,
        mesh=torus,
        in_specs=(P(None, (X, Z), (Y, CORE)), P(None, (X, Z), (Y, CORE)), P((Y, CORE))),
        out_specs=P(None, (X, Z), (Y, CORE)),
        check_vma=False,
    )
```
